256 devices in a mesh: tm: 64 (over z_lo, y, x, core), space: 4 (over z_hi).
Axes of the slice: x: 4, y: 4, z: 8 (z_hi: 4, z_lo: 2; z = z_hi * 2 + z_lo), core: 2. Of those that a mesh axis runs over, the one named last changes fastest.
Arguments:
- rhs: float32 [128, 1024, 1024], P('tm', 'space'), may hold values from -6 to 6
- guess: float32 [128, 1024, 1024], P('tm', 'space'), may hold values from -6 to 6
- diffusion: float32 [1024, 1024], P('space'), may hold values from 0.2 to 2
Outputs:
- solution: float32 [128, 1024, 1024], P('tm', 'space')
- norms: float32 [6], replicated
The draws below stay inside these ranges and needn't reach their ends.
All inputs are finite; a program needn't handle non-finite values.
Results may differ from the reference program's by a relative error of at most 0.0001.
Values sent between devices are 32-bit elements; how exact they have to be, the bound alone decides.
A program may use at most 64 MiB of HBM per device.

```python
import math
import jax
import jax.numpy as jnp

NY = 1024
LEVELS = 5
NT = 128
NX = 1024


def levels(own_key, extent, split, smallest, high):
    loudness = 1.0
    for dim, shards_of in split:
        steps = jax.random.uniform(jax.random.fold_in(jax.random.fold_in(own_key, 6), dim), (shards_of,), jnp.float32, smallest / len(split), high / len(split))
        loudness = loudness * jnp.repeat(jnp.exp(steps), extent[dim] // shards_of).reshape((-1,) + (1,) * (len(extent) - 1 - dim))
    return loudness


def centred(rng, dims, spread, limit, pieces=(), held_as=jnp.bfloat16):
    gain = levels(rng, dims, pieces, -0.22, 0.18) if pieces else 1.0
    values = jax.random.normal(rng, dims, jnp.float32) * spread * gain
    return jnp.minimum(jnp.maximum(values, -limit), limit).astype(held_as)


def setup_inputs(seed: int = 0) -> dict:
    streams_of = jax.random.split(jax.random.key(seed), 4)
    rhs = centred(streams_of[0], (NT, NX, NY), 1.0, 6.0, ((0, 64), (1, 4)), jnp.float32)
    guess = centred(streams_of[1], (NT, NX, NY), 1.0, 6.0, ((0, 64), (1, 4)), jnp.float32)
    diffusion = jnp.clip(jnp.exp(math.log(2.0) - 2.3025851 * jax.random.uniform(streams_of[2], (NX, NY), jnp.float32) ** levels(streams_of[2], (NX, NY), ((0, 4),), -0.2, 0.2)), 0.2, 2.0)
    return dict(rhs=rhs, guess=guess, diffusion=diffusion)


def neighbours(field):
    padded = jnp.pad(field, ((0, 0), (1, 1), (1, 1)))
    total = padded[:, 2:, 1:-1] + padded[:, :-2, 1:-1]
    total = total + padded[:, 1:-1, 2:] + padded[:, 1:-1, :-2]
    return total

def residual(field, source, scaled, diag):
    before = jnp.concatenate([jnp.zeros_like(field[:1]), field[:-1]], axis=0)
    image = diag * field - scaled * neighbours(field) - before
    return source - image

def reference(rhs, guess, diffusion):
    damping = 0.8
    cells = rhs.shape[1] * rhs.shape[2]
    squares = []
    sources = [rhs]
    fields = []
    field = guess
    for level in range(LEVELS - 1):
        source = sources[level]
        scaled = 2.0 ** level * diffusion
        diag = 1.0 + 4.0 * scaled
        if level == 0:
            field = field + damping * residual(field, source, scaled, diag) / diag
        else:
            field = damping * source / diag
        resid = residual(field, source, scaled, diag)
        squares.append(jnp.sum(resid * resid))
        fields.append(field)
        sources.append(resid[0::2] + resid[1::2])
    level = LEVELS - 1
    source = sources[level]
    scaled = 2.0 ** level * diffusion
    diag = 1.0 + 4.0 * scaled
    field = damping * source / diag
    field = field + damping * residual(field, source, scaled, diag) / diag
    resid = residual(field, source, scaled, diag)
    squares.append(jnp.sum(resid * resid))
    correction = field
    for level in range(LEVELS - 2, -1, -1):
        scaled = 2.0 ** level * diffusion
        diag = 1.0 + 4.0 * scaled
        field = fields[level] + jnp.repeat(correction, 2, axis=0)
        field = field + damping * residual(field, sources[level], scaled, diag) / diag
        correction = field
    scaled = 1.0 * diffusion
    diag = 1.0 + 4.0 * scaled
    resid = residual(correction, rhs, scaled, diag)
    squares.append(jnp.sum(resid * resid))
    norms = jnp.sqrt(jnp.stack(squares) / cells)
    return (correction, norms)
```

```python
import jax
import jax.numpy as jnp
from jax import lax
from jax.sharding import Mesh
from jax.sharding import PartitionSpec as P

LEVELS = 5
TM = ("tm_0", "tm_1", "tm_2", "tm_3")
TM_SPACE = ("tm_0", "tm_1", "tm_2", "tm_3", "space")


damping = 0.8


def with_halo(block, sides, width):
    for axis, dim in sides:
        count = lax.axis_size(axis)
        forward = [(i, i + 1) for i in range(count - 1)]
        backward = [(target, source) for source, target in forward]
        low = lax.ppermute(
            lax.slice_in_dim(block, block.shape[dim] - width, None, axis=dim), axis, forward
        )
        high = lax.ppermute(lax.slice_in_dim(block, 0, width, axis=dim), axis, backward)
        block = jnp.concatenate([low, block, high], axis=dim)
    return block


def shifted(value, axis, steps):
    count = lax.axis_size(axis)
    first, last = (max(0, -steps), min(count, count - steps))
    return lax.ppermute(value, axis, [(source, source + steps) for source in range(first, last)])


def from_partner(value, axis, apart):
    mask = 2**apart
    pairs = [(source, source ^ mask) for source in range(lax.axis_size(axis))]
    return lax.ppermute(value, axis, pairs)


def over_axes(array, axes):
    return lax.psum(array, axes)


def neighbours(field):
    rows = with_halo(field, (("space", 1),), 1)
    padded = jnp.pad(rows, ((0, 0), (0, 0), (1, 1)))
    total = padded[:, 2:, 1:-1] + padded[:, :-2, 1:-1]
    total = total + padded[:, 1:-1, 2:] + padded[:, 1:-1, :-2]
    return total


def residual(field, source, scaled, diag, stride):
    earlier = shifted(field[-1:], TM, stride)
    before = jnp.concatenate([earlier, field[:-1]], axis=0)
    image = diag * field - scaled * neighbours(field) - before
    return source - image


def stride_of(level):
    if level == 0:
        return 1
    return 2 ** (level - 1)


def body(rhs, guess, diffusion):
    position = lax.axis_index(TM)
    cells = rhs.shape[1] * lax.axis_size("space") * rhs.shape[2]
    partials = []

    def weight_of(level):
        if level <= 1:
            return jnp.float32(1.0)
        stride = stride_of(level)
        return jnp.where(position % stride == stride - 1, 1.0, 0.0).astype(jnp.float32)

    def record(resid, level):
        local_part = jnp.sum(resid * resid) * weight_of(level)
        partials.append(local_part)

    sources = [rhs]
    fields = []
    field = guess
    for level in range(LEVELS - 1):
        source = sources[level]
        scaled = 2.0**level * diffusion
        diag = 1.0 + 4.0 * scaled
        stride = stride_of(level)
        if level == 0:
            field = field + damping * residual(field, source, scaled, diag, stride) / diag
        else:
            field = damping * source / diag
        resid = residual(field, source, scaled, diag, stride)
        record(resid, level)
        fields.append(field)
        if level == 0:
            coarse = resid[0:1] + resid[1:2]
        else:
            coarse = resid + from_partner(resid, TM, level - 1)
        sources.append(coarse)
    level = LEVELS - 1
    source = sources[level]
    scaled = 2.0**level * diffusion
    diag = 1.0 + 4.0 * scaled
    stride = stride_of(level)
    field = damping * source / diag
    field = field + damping * residual(field, source, scaled, diag, stride) / diag
    resid = residual(field, source, scaled, diag, stride)
    record(resid, level)
    correction = field
    for level in range(LEVELS - 2, -1, -1):
        scaled = 2.0**level * diffusion
        diag = 1.0 + 4.0 * scaled
        stride = stride_of(level)
        field = fields[level] + correction
        field = field + damping * residual(field, sources[level], scaled, diag, stride) / diag
        correction = field
    scaled = 1.0 * diffusion
    diag = 1.0 + 4.0 * scaled
    resid = residual(correction, rhs, scaled, diag, 1)
    record(resid, 0)
    totals = over_axes(jnp.stack(partials), TM_SPACE)
    norms = jnp.sqrt(totals / cells)
    return (correction, norms)


def solution(mesh):
    split = Mesh(
        mesh.devices.reshape(2, 4, 4, 2, mesh.shape["space"]),
        ("tm_0", "tm_1", "tm_2", "tm_3", "space"),
    )
    return jax.shard_map(
        body,
        mesh=split,
        in_specs=(P(TM, "space", None), P(TM, "space", None), P("space", None)),
        out_specs=(P(TM, "space", None), P()),
        check_vma=False,
    )
```

```python
import jax
import jax.numpy as jnp
from jax import lax
from jax.experimental import pallas as pl
from jax.experimental.pallas import tpu as pltpu
from jax.sharding import PartitionSpec as P

MESH = pl.DeviceIdType.MESH
f32 = jnp.float32
GROUP = 32
HALVES = 2
STRIPS = 4
TILES = 32
EXT = TILES + 2
COLS = 1024
CELLS = 1048576.0
POINTS = {1: 32, 2: 16, 3: 8, 4: 4}


def snake(j):
    y = j // 8
    x = (j // 2) % 4
    x = x + (y % 2) * (3 - 2 * x)
    return (y * 4 + x) * 2 + j % 2


def kernel(rhs, guess, diff, out, norms, sc):
    m = lax.axis_index("tm")
    s = lax.axis_index("space")
    j = m % GROUP
    h = m // GROUP
    odd = s % 2

    def rank_of(b):
        return snake(b + odd * (TILES - 1 - 2 * b))

    place = snake(j)
    b = place + odd * (TILES - 1 - 2 * place)
    first = (TILES - 1 - b) // (TILES - 1)
    last = b // (TILES - 1)
    up_id = (h * GROUP + rank_of(b - 1 + first), (s - first + STRIPS) % STRIPS)
    dn_id = (h * GROUP + rank_of(b + 1 - last), (s + last) % STRIPS)
    has_up = b + s > 0
    has_dn = b + s < TILES + STRIPS - 2
    next_id = ((m + 1) % (GROUP * HALVES), s)
    half_id = ((m + GROUP) % (GROUP * HALVES), s)
    north_id = (m, (s + STRIPS - 1) % STRIPS)
    south_id = (m, (s + 1) % STRIPS)
    has_next = m < GROUP * HALVES - 1
    has_prev = m > 0

    row = lax.broadcasted_iota(jnp.int32, (8, COLS), 0)
    col = lax.broadcasted_iota(jnp.int32, (8, COLS), 1)

    def nb(tile, above, below):
        up = pltpu.roll(jnp.where(row == 7, above, tile), 1, 0)
        down = pltpu.roll(jnp.where(row == 0, below, tile), 7, 0)
        left = jnp.where(col == 0, 0.0, pltpu.roll(tile, 1, 1))
        right = jnp.where(col == COLS - 1, 0.0, pltpu.roll(tile, COLS - 1, 1))
        return (up + down) + (left + right)

    def around(ref, i):
        return nb(ref[i], ref[i - 1 + (EXT - 1 - i) // (EXT - 1)], ref[i + 1 - i // (EXT - 1)])

    def tiles(lo, hi, fn):
        def step(i, carry):
            fn(i)
            return carry

        lax.fori_loop(lo, hi, step, 0)

    def remote(src, dst, send, recv, device):
        return pltpu.make_async_remote_copy(
            src_ref=src, dst_ref=dst, send_sem=send, recv_sem=recv,
            device_id=device, device_id_type=MESH,
        )

    def when(cond, fn):
        pl.when(cond)(fn)

    fe, ge, de, ee = sc["fe"], sc["ge"], sc["de"], sc["ee"]
    va, vb, ra, rb = sc["va"], sc["vb"], sc["ra"], sc["rb"]
    uo, ui, pe, xo, xi, vp = sc["uo"], sc["ui"], sc["pe"], sc["xo"], sc["xi"], sc["vp"]
    wo, n1, np_ = sc["wo"], sc["n1"], sc["np"]

    inner = pl.ds(1, TILES)
    loads = [
        pltpu.make_async_copy(guess.at[1], ge.at[1, inner], sc["load"].at[0]),
        pltpu.make_async_copy(diff, de.at[inner], sc["load"].at[1]),
        pltpu.make_async_copy(guess.at[0], ge.at[0, inner], sc["load"].at[2]),
        pltpu.make_async_copy(rhs, fe.at[:, inner], sc["load"].at[3]),
    ]
    for load in loads:
        load.start()

    barrier = pltpu.get_barrier_semaphore()

    def greet(device):
        pl.semaphore_signal(barrier, inc=1, device_id=device, device_id_type=MESH)

    def greet_rank(r, carry):
        greet((h * GROUP + (j + r) % GROUP, s))
        return carry

    lax.fori_loop(1, GROUP, greet_rank, 0)
    mine = h * STRIPS + s

    def greet_other(r, carry):
        other = (mine + r) % (HALVES * STRIPS)
        greet(((other // STRIPS) * GROUP + j, other % STRIPS))
        return carry

    lax.fori_loop(1, HALVES * STRIPS, greet_other, 0)
    when(m == GROUP - 1, lambda: greet((GROUP, s)))
    when(m == GROUP, lambda: greet((GROUP - 1, s)))
    peers = GROUP - 1 + HALVES * STRIPS - 1
    seam = (m == GROUP - 1) | (m == GROUP)
    when(seam, lambda: pl.semaphore_wait(barrier, peers + 1))
    when(jnp.logical_not(seam), lambda: pl.semaphore_wait(barrier, peers))
    for load in loads:
        load.wait()

    halo = []
    for k, ref in enumerate((ge.at[1], de, ge.at[0], fe.at[0], fe.at[1])):
        halo.append((
            remote(ref.at[1], ref.at[EXT - 1], sc["hs"].at[k, 0], sc["hr"].at[k, 0], north_id),
            remote(ref.at[TILES], ref.at[0], sc["hs"].at[k, 1], sc["hr"].at[k, 1], south_id),
        ))
    for north, south in halo:
        when(s > 0, north.start)
        when(s < STRIPS - 1, south.start)

    zero = jnp.zeros((8, COLS), f32)

    def outside(at):
        for ref in (ge.at[1], de, ge.at[0], fe.at[0], fe.at[1], n1):
            ref[at] = zero

    when(s == 0, lambda: outside(0))
    when(s == STRIPS - 1, lambda: outside(EXT - 1))

    def no_prev():
        def clear(i):
            for ref in (ui, pe, xi, np_):
                ref[i] = zero

        tiles(0, EXT, clear)

    when(m == 0, no_prev)

    def no_half():
        for name in ("v1", "v2", "v3", "v4a", "v4b", "n3", "n2"):
            sc[name][0] = zero

    when(h == 0, no_half)

    def damp(i):
        ee[i] = 0.8 / (1.0 + 4.0 * de[i])

    def sweep0(i):
        e, d = ee[i], de[i]
        a, bb = ge[0, i], ge[1, i]
        va[i] = 0.2 * a + e * (fe[0, i] + d * around(ge.at[0], i))
        vb[i] = 0.2 * bb + e * (fe[1, i] + d * around(ge.at[1], i) + a)
        wo[i] = e * bb

    def give(i):
        w = wo[i]
        uo[i] = (vb[i] - 0.8 * ge[1, i]) + (de[i] * around(wo, i) + w)

    tiles(1, TILES + 1, damp)
    tiles(2, TILES, sweep0)
    tiles(3, TILES - 1, give)
    spans = ((3, 14), (17, 14), (0, 3), (31, 3))
    give_copies = []
    for k, (lo, n) in enumerate(spans):
        at = pl.ds(lo, n)
        give_copies.append(remote(uo.at[at], ui.at[at], sc["us"].at[k], sc["ur"].at[k], next_id))
    when(has_next, give_copies[0].start)
    when(has_next, give_copies[1].start)

    for north, south in halo:
        when(s > 0, north.wait_send)
        when(s < STRIPS - 1, north.wait_recv)
        when(s < STRIPS - 1, south.wait_send)
        when(s > 0, south.wait_recv)
    damp(0)
    damp(EXT - 1)

    def no_row(at):
        ee[at] = zero

    when(s == 0, lambda: no_row(0))
    when(s == STRIPS - 1, lambda: no_row(EXT - 1))
    tiles(0, 2, sweep0)
    tiles(TILES, EXT, sweep0)
    tiles(0, 3, give)
    tiles(TILES - 1, EXT, give)
    when(has_next, give_copies[2].start)
    when(has_next, give_copies[3].start)

    g1, go = sc["g1"], sc["go"]

    def resid0(i):
        d = de[i]
        diag = 1.0 + 4.0 * d
        a, bb = va[i], vb[i]
        ra[i] = (fe[0, i] - diag * a) + d * around(va, i)
        rb[i] = (fe[1, i] - diag * bb) + (d * around(vb, i) + a)

    tiles(1, TILES + 1, resid0)

    def scatter(i):
        g = (ra[i] + rb[i]) + ui[i]
        go[i - 1] = g
        rank = rank_of(i - 1)

        def keep():
            g1[j] = g

        when(rank == j, keep)
        copy = remote(go.at[i - 1], g1.at[j], sc["gs"], sc["gr"], (h * GROUP + rank, s))
        when(rank != j, copy.start)

    for copy, (lo, n) in zip(give_copies, spans):
        when(has_prev, copy.wait_recv)
        tiles(max(lo, 1), min(lo + n, TILES + 1), scatter)

    dm = de[b + 1]
    for level in range(1, 5):
        sc["em"][level - 1] = 0.8 / (1.0 + 4.0 * (2.0**level * dm))
        sc["sm"][level - 1] = 2.0**level * dm
    all_in = remote(go.at[pl.ds(0, GROUP - 1)], g1.at[pl.ds(0, GROUP - 1)], sc["gs"], sc["gr"], next_id)
    all_in.wait_recv()

    def exchange(k, name, count):
        v = sc[name]
        return (
            (has_up, has_dn, remote(sc["st" + name], sc["hb" + name], sc["xs"].at[k, 0], sc["xr"].at[k, 0], up_id)),
            (has_dn, has_up, remote(sc["sb" + name], sc["ht" + name], sc["xs"].at[k, 1], sc["xr"].at[k, 1], dn_id)),
            (h == 0, h == 1, remote(v.at[count], v.at[0], sc["xs"].at[k, 2], sc["xr"].at[k, 2], half_id)),
        )

    def start(copies):
        for sends, _, copy in copies:
            when(sends, copy.start)

    def land(copies):
        for sends, takes, copy in copies:
            when(takes, copy.wait_recv)
            when(sends, copy.wait_send)

    def store(name, p, value):
        sc[name][p + 1] = value
        sc["st" + name][p] = value[0:1]
        sc["sb" + name][p] = value[7:8]

    for name, level in (("v1", 1), ("v2", 2), ("v3", 3), ("v4a", 4), ("v4b", 4), ("n3", 3), ("n2", 2)):
        def no_top(name=name, level=level):
            def clear(p):
                sc["ht" + name][p] = jnp.zeros((1, COLS), f32)

            tiles(0, POINTS[level], clear)

        def no_bottom(name=name, level=level):
            def clear(p):
                sc["hb" + name][p] = jnp.zeros((1, COLS), f32)

            tiles(0, POINTS[level], clear)

        when(b + s == 0, no_top)
        when(b + s == TILES + STRIPS - 2, no_bottom)

    parts = ((0, 9), (9, 9), (18, 8), (26, 8))
    p_copies = []
    x_copies = []
    for k, (lo, n) in enumerate(parts):
        at = pl.ds(lo, n)
        p_copies.append(remote(ge.at[1, at], pe.at[at], sc["ps"].at[k], sc["pr"].at[k], next_id))
        x_copies.append(remote(xo.at[at], xi.at[at], sc["qs"].at[k], sc["qr"].at[k], next_id))

    sources = {1: g1, 2: sc["g2"], 3: sc["g3"], 4: sc["g4"]}
    squares = {}

    def first_sweep(p):
        store("v1", p, sc["em"][0] * g1[p])

    tiles(0, POINTS[1], first_sweep)
    copies = exchange(0, "v1", POINTS[1])
    start(copies)
    when(has_next, p_copies[0].start)
    names = {1: "v1", 2: "v2", 3: "v3", 4: "v4a"}
    for level in (1, 2, 3):
        land(copies)
        name = names[level]
        v, ht, hb, g = sc[name], sc["ht" + name], sc["hb" + name], sources[level]
        coarse, below = sources[level + 1], names[level + 1]
        sl = level - 1

        def descend(q, acc):
            scaled = sc["sm"][sl]
            before, now, after = v[2 * q], v[2 * q + 1], v[2 * q + 2]
            p = 2 * q
            r0 = (0.2 * g[p] + scaled * nb(now, ht[p], hb[p])) + before
            r1 = (0.2 * g[p + 1] + scaled * nb(after, ht[p + 1], hb[p + 1])) + now
            total = r0 + r1
            coarse[q] = total
            store(below, q, sc["em"][sl + 1] * total)
            return acc + (r0 * r0 + r1 * r1)

        squares[level] = lax.fori_loop(0, POINTS[level + 1], descend, zero)
        sc["acc"][level] = squares[level]
        copies = exchange(level, below, POINTS[level + 1])
        start(copies)
        when(has_next, p_copies[level].start)
    land(copies)

    def second_sweep(p, carry):
        v = sc["v4a"]
        now = v[p + 1]
        new = 0.2 * now + sc["em"][3] * (
            sc["g4"][p] + sc["sm"][3] * nb(now, sc["htv4a"][p], sc["hbv4a"][p]) + v[p]
        )
        store("v4b", p, new)
        return carry

    lax.fori_loop(0, POINTS[4], second_sweep, 0)
    copies = exchange(4, "v4b", POINTS[4])
    start(copies)

    for copy in p_copies:
        when(has_prev, copy.wait_recv)

    def complete(i):
        w = ee[i] * pe[i]
        va[i] = va[i] + w
        xo[i] = w

    tiles(0, EXT, complete)

    def carry_over(i, acc):
        w = xo[i]
        u = ui[i]
        vp[i] = ((u - w) + 0.8 * pe[i]) - de[i] * around(xo, i)
        return acc

    lax.fori_loop(0, EXT, carry_over, 0)

    def energy(i, acc):
        w = xo[i]
        r0 = ra[i] + (ui[i] - w)
        r1 = rb[i] + w
        return acc + (r0 * r0 + r1 * r1)

    sc["acc"][0] = lax.fori_loop(1, TILES + 1, energy, zero)

    def hand_on(i):
        xo[i] = 0.2 * vb[i] + ee[i] * (fe[1, i] + de[i] * around(vb, i) + va[i])

    tiles(0, EXT, hand_on)

    land(copies)

    def last_resid(p, acc):
        v = sc["v4b"]
        now, g = v[p + 1], sc["g4"][p]
        scaled = sc["sm"][3]
        r = (g - (1.0 + 4.0 * scaled) * now) + (
            scaled * nb(now, sc["htv4b"][p], sc["hbv4b"][p]) + v[p]
        )
        return acc + r * r

    sc["acc"][4] = lax.fori_loop(0, POINTS[4], last_resid, zero)

    no = sc["no"]
    above = "v4b"
    for level, name, k in ((3, "n3", 5), (2, "n2", 6), (1, None, None)):
        low = names[level]
        v, ht, hb, g = sc[low], sc["ht" + low], sc["hb" + low], sources[level]
        c, ct, cb = sc[above], sc["ht" + above], sc["hb" + above]
        sl = level - 1

        def ascend(q, carry):
            scaled, e = sc["sm"][sl], sc["em"][sl]
            this = c[q + 1]
            top, bottom = ct[q], cb[q]
            before = v[2 * q] + c[q]
            for i in range(2):
                p = 2 * q + i
                now = v[p + 1] + this
                around_it = nb(now, ht[p] + top, hb[p] + bottom)
                new = 0.2 * now + e * (g[p] + scaled * around_it + before)
                before = now
                if name is None:
                    no[p] = new
                else:
                    store(name, p, new)
            return carry

        lax.fori_loop(0, POINTS[level] // 2, ascend, 0)
        if name is None:
            break
        copies = exchange(k, name, POINTS[level])
        start(copies)
        for copy in x_copies[2 * (k - 5):2 * (k - 5) + 2]:
            when(has_next, copy.start)
        land(copies)
        above = name

    def back(p):
        copy = remote(no.at[p], n1.at[b + 1], sc["bs"], sc["br"].at[b], (h * GROUP + p, s))

        def keep():
            n1[b + 1] = no[p]

        when(p == j, keep)
        when(p != j, copy.start)

    tiles(0, GROUP, back)

    def forward(tile):
        return remote(n1.at[tile], np_.at[tile], sc["fs"], sc["fr"], next_id)

    edge_north = remote(n1.at[1], n1.at[EXT - 1], sc["es"].at[0], sc["er"].at[0], north_id)
    edge_south = remote(n1.at[TILES], n1.at[0], sc["es"].at[1], sc["er"].at[1], south_id)

    def arrive(i, carry):
        copy = remote(n1.at[i + 1], n1.at[i + 1], sc["bs"], sc["br"].at[i], next_id)
        when(i != b, copy.wait_recv)
        when(has_next, forward(i + 1).start)
        return carry

    lax.fori_loop(0, 1, arrive, 0)
    when(s > 0, edge_north.start)
    lax.fori_loop(TILES - 1, TILES, arrive, 0)
    when(s < STRIPS - 1, edge_south.start)
    lax.fori_loop(1, TILES - 1, arrive, 0)
    when(s < STRIPS - 1, edge_north.wait_recv)
    when(s > 0, edge_south.wait_recv)
    when(has_next, forward(0).start)
    when(has_next, forward(EXT - 1).start)

    def correct(i):
        t = n1[i]
        va[i] = va[i] + t
        vb[i] = vb[i] + t

    tiles(0, EXT, correct)

    for copy in x_copies:
        when(has_prev, copy.wait_recv)
    whole = remote(n1, np_, sc["fs"], sc["fr"], next_id)
    when(has_prev, whole.wait_recv)

    def last_sweep(i):
        e, d = ee[i], de[i]
        a, bb = va[i], vb[i]
        ra[i] = 0.2 * a + e * (fe[0, i] + d * around(va, i) + (vp[i] + np_[i]))
        rb[i] = 0.2 * bb + e * (fe[1, i] + d * around(vb, i) + a)

    tiles(0, EXT, last_sweep)
    writes = [
        pltpu.make_async_copy(ra.at[inner], out.at[0], sc["write"].at[0]),
        pltpu.make_async_copy(rb.at[inner], out.at[1], sc["write"].at[1]),
    ]
    for write in writes:
        write.start()

    def final(i, acc):
        e, d = ee[i], de[i]
        diag = 1.0 + 4.0 * d
        a, bb, t = ra[i], rb[i], np_[i]
        before = xi[i] + (0.2 * t + e * (d * around(np_, i) + t))
        r0 = (fe[0, i] - diag * a) + (d * around(ra, i) + before)
        r1 = (fe[1, i] - diag * bb) + (d * around(rb, i) + a)
        return acc + (r0 * r0 + r1 * r1)

    sc["acc"][5] = lax.fori_loop(1, TILES + 1, final, zero)

    lines = lax.broadcasted_iota(jnp.int32, (8, 128), 0)
    part = jnp.zeros((8, 128), f32)
    for k in range(6):
        whole_sum = sc["acc"][k]
        narrow = whole_sum[:, 0:128]
        for c in range(1, COLS // 128):
            narrow = narrow + whole_sum[:, c * 128:(c + 1) * 128]
        part = jnp.where(lines == k, jnp.sum(narrow, axis=0, keepdims=True), part)
    sc["t0"][...] = part
    sc["q0"][j] = part

    def tell(r, carry):
        copy = remote(sc["t0"], sc["q0"].at[j], sc["ns"].at[0], sc["nr"].at[0], (h * GROUP + (j + r) % GROUP, s))
        copy.start()
        return carry

    lax.fori_loop(1, GROUP, tell, 0)
    heard = remote(sc["q0"].at[pl.ds(0, GROUP - 1)], sc["q0"].at[pl.ds(0, GROUP - 1)], sc["ns"].at[0], sc["nr"].at[0], next_id)
    heard.wait_recv()
    part = sc["q0"][0]
    for k in range(1, GROUP):
        part = part + sc["q0"][k]
    sc["t1"][...] = part
    sc["q1"][mine] = part

    def tell_far(r, carry):
        other = (mine + r) % (HALVES * STRIPS)
        device = ((other // STRIPS) * GROUP + j, other % STRIPS)
        remote(sc["t1"], sc["q1"].at[mine], sc["ns"].at[1], sc["nr"].at[1], device).start()
        return carry

    lax.fori_loop(1, HALVES * STRIPS, tell_far, 0)
    far = pl.ds(0, HALVES * STRIPS - 1)
    heard_far = remote(sc["q1"].at[far], sc["q1"].at[far], sc["ns"].at[1], sc["nr"].at[1], next_id)
    heard_far.wait_recv()
    part = sc["q1"][0]
    for k in range(1, HALVES * STRIPS):
        part = part + sc["q1"][k]
    total = jnp.sum(part, axis=1, keepdims=True)
    norms[...] = jnp.broadcast_to(jnp.sqrt(total / CELLS), (8, 128))

    for copy in give_copies + p_copies + x_copies:
        when(has_next, copy.wait_send)
    all_in.wait_send()
    remote(no.at[pl.ds(0, GROUP - 1)], no.at[pl.ds(0, GROUP - 1)], sc["bs"], sc["br"].at[0], next_id).wait_send()
    when(has_next, whole.wait_send)
    when(s > 0, edge_north.wait_send)
    when(s < STRIPS - 1, edge_south.wait_send)
    heard.wait_send()
    heard_far.wait_send()
    for write in writes:
        write.wait()


def scratch():
    ext = pltpu.VMEM((EXT, 8, COLS), f32)
    shapes = {"fe": pltpu.VMEM((2, EXT, 8, COLS), f32), "ge": pltpu.VMEM((2, EXT, 8, COLS), f32)}
    for name in ("de", "ee", "va", "vb", "ra", "rb", "uo", "ui", "pe", "xo", "xi", "vp", "wo", "n1", "np"):
        shapes[name] = ext
    for name in ("g1", "go", "no"):
        shapes[name] = pltpu.VMEM((GROUP, 8, COLS), f32)
    for name, level in (("g2", 2), ("g3", 3), ("g4", 4)):
        shapes[name] = pltpu.VMEM((POINTS[level], 8, COLS), f32)
    for name, level in (("v1", 1), ("v2", 2), ("v3", 3), ("v4a", 4), ("v4b", 4), ("n3", 3), ("n2", 2)):
        shapes[name] = pltpu.VMEM((POINTS[level] + 1, 8, COLS), f32)
        for side in ("st", "sb", "ht", "hb"):
            shapes[side + name] = pltpu.VMEM((POINTS[level], 1, COLS), f32)
    shapes["em"] = shapes["sm"] = pltpu.VMEM((4, 8, COLS), f32)
    shapes["acc"] = pltpu.VMEM((6, 8, COLS), f32)
    shapes["t0"] = shapes["t1"] = pltpu.VMEM((8, 128), f32)
    shapes["q0"] = pltpu.VMEM((GROUP, 8, 128), f32)
    shapes["q1"] = pltpu.VMEM((HALVES * STRIPS, 8, 128), f32)
    for name, dims in (
        ("load", (4,)), ("hs", (5, 2)), ("hr", (5, 2)), ("us", (4,)), ("ur", (4,)),
        ("gs", ()), ("gr", ()), ("xs", (7, 3)), ("xr", (7, 3)), ("ps", (4,)), ("pr", (4,)),
        ("qs", (4,)), ("qr", (4,)), ("bs", ()), ("br", (TILES,)), ("fs", ()), ("fr", ()),
        ("es", (2,)), ("er", (2,)), ("ns", (2,)), ("nr", (2,)), ("write", (2,)),
    ):
        shapes[name] = pltpu.SemaphoreType.DMA(dims)
    return shapes


def body(rhs, guess, diffusion):
    anywhere = pl.BlockSpec(memory_space=pl.ANY)
    field, norms = pl.pallas_call(
        kernel,
        out_shape=(
            jax.ShapeDtypeStruct((2, TILES, 8, COLS), f32),
            jax.ShapeDtypeStruct((8, 128), f32),
        ),
        in_specs=[anywhere] * 3,
        out_specs=(anywhere, pl.BlockSpec(memory_space=pltpu.VMEM)),
        scratch_shapes=[scratch()],
        compiler_params=pltpu.CompilerParams(collective_id=0, has_side_effects=True, vmem_limit_bytes=60000 * 1024),
        name="cycle",
    )(
        rhs.reshape(2, TILES, 8, COLS),
        guess.reshape(2, TILES, 8, COLS),
        diffusion.reshape(TILES, 8, COLS),
    )
    return field.reshape(2, TILES * 8, COLS), norms[:6, 0]


def solution(mesh):
    return jax.shard_map(
        body,
        mesh=mesh,
        in_specs=(P("tm", "space", None), P("tm", "space", None), P("space", None)),
        out_specs=(P("tm", "space", None), P()),
        check_vma=False,
    )
```

```python
import jax
import jax.numpy as jnp
from jax import lax
from jax.experimental import pallas as pl
from jax.experimental.pallas import tpu as pltpu
from jax.sharding import PartitionSpec as P

MESH = pl.DeviceIdType.MESH
f32 = jnp.float32
GROUP = 32
HALVES = 2
STRIPS = 4
TILES = 32
EXT = TILES + 2
COLS = 1024
CELLS = 1048576.0
POINTS = {1: 32, 2: 16, 3: 8, 4: 4}


def snake(j):
    y = j // 8
    x = (j // 2) % 4
    x = x + (y % 2) * (3 - 2 * x)
    return (y * 4 + x) * 2 + j % 2


def kernel(rhs, guess, diff, out, norms, sc):
    m = lax.axis_index("tm")
    s = lax.axis_index("space")
    j = m % GROUP
    h = m // GROUP
    odd = s % 2

    def mirror(j, h):
        return j + h * 8 * (3 - 2 * (j // 8))

    def rank_of(b, h=h):
        return mirror(snake(b + odd * (TILES - 1 - 2 * b)), h)

    place = snake(mirror(j, h))
    b = place + odd * (TILES - 1 - 2 * place)
    first = (TILES - 1 - b) // (TILES - 1)
    last = b // (TILES - 1)
    up_id = (h * GROUP + rank_of(b - 1 + first), (s - first + STRIPS) % STRIPS)
    dn_id = (h * GROUP + rank_of(b + 1 - last), (s + last) % STRIPS)
    has_up = b + s > 0
    has_dn = b + s < TILES + STRIPS - 2
    next_id = ((m + 1) % (GROUP * HALVES), s)
    half_id = ((1 - h) * GROUP + rank_of(b, 1 - h), s)
    north_id = (m, (s + STRIPS - 1) % STRIPS)
    south_id = (m, (s + 1) % STRIPS)
    has_next = m < GROUP * HALVES - 1
    has_prev = m > 0

    row = lax.broadcasted_iota(jnp.int32, (8, COLS), 0)
    col = lax.broadcasted_iota(jnp.int32, (8, COLS), 1)

    def nb(tile, above, below):
        up = pltpu.roll(jnp.where(row == 7, above, tile), 1, 0)
        down = pltpu.roll(jnp.where(row == 0, below, tile), 7, 0)
        left = jnp.where(col == 0, 0.0, pltpu.roll(tile, 1, 1))
        right = jnp.where(col == COLS - 1, 0.0, pltpu.roll(tile, COLS - 1, 1))
        return (up + down) + (left + right)

    def around(ref, i):
        return nb(ref[i], ref[i - 1 + (EXT - 1 - i) // (EXT - 1)], ref[i + 1 - i // (EXT - 1)])

    def tiles(lo, hi, fn):
        def step(i, carry):
            fn(i)
            return carry

        lax.fori_loop(lo, hi, step, 0)

    def remote(src, dst, send, recv, device):
        return pltpu.make_async_remote_copy(
            src_ref=src, dst_ref=dst, send_sem=send, recv_sem=recv,
            device_id=device, device_id_type=MESH,
        )

    def when(cond, fn):
        pl.when(cond)(fn)

    fe, ge, de, ee = sc["fe"], sc["ge"], sc["de"], sc["ee"]
    va, vb, ra, rb = sc["va"], sc["vb"], sc["ra"], sc["rb"]
    uo, ui, pe, xo, xi, vp = sc["uo"], sc["ui"], sc["pe"], sc["xo"], sc["xi"], sc["vp"]
    wo, n1, np_ = sc["wo"], sc["n1"], sc["np"]

    inner = pl.ds(1, TILES)
    loads = [
        pltpu.make_async_copy(guess.at[1], ge.at[1, inner], sc["load"].at[0]),
        pltpu.make_async_copy(diff, de.at[inner], sc["load"].at[1]),
        pltpu.make_async_copy(guess.at[0], ge.at[0, inner], sc["load"].at[2]),
        pltpu.make_async_copy(rhs, fe.at[:, inner], sc["load"].at[3]),
    ]
    for load in loads:
        load.start()

    barrier = pltpu.get_barrier_semaphore()

    def greet(device):
        pl.semaphore_signal(barrier, inc=1, device_id=device, device_id_type=MESH)

    def greet_rank(r, carry):
        greet((h * GROUP + (j + r) % GROUP, s))
        return carry

    lax.fori_loop(1, GROUP, greet_rank, 0)
    mine = h * STRIPS + s

    def greet_other(r, carry):
        other = (mine + r) % (HALVES * STRIPS)
        greet(((other // STRIPS) * GROUP + j, other % STRIPS))
        return carry

    lax.fori_loop(1, HALVES * STRIPS, greet_other, 0)
    greet(half_id)
    def greet_first_half():
        def greet_one(r, carry):
            greet((r, s))
            return carry

        lax.fori_loop(1, GROUP, greet_one, 0)

    when(m == GROUP, greet_first_half)

    zero = jnp.zeros((8, COLS), f32)

    def outside(at):
        for ref in (ge.at[1], de, ge.at[0], fe.at[0], fe.at[1], n1):
            ref[at] = zero

    when(s == 0, lambda: outside(0))
    when(s == STRIPS - 1, lambda: outside(EXT - 1))

    def no_prev():
        def clear(i):
            for ref in (ui, pe, xi, np_):
                ref[i] = zero

        tiles(0, EXT, clear)

    when(m == 0, no_prev)

    def no_half():
        sc["v1"][0] = zero
        for name in ("v2", "v3", "v4a", "v4b", "n3", "n2"):
            for t in range(3):
                sc[name][0, t] = zero

    when(h == 0, no_half)

    def no_top():
        def clear(p):
            sc["ht"][p] = jnp.zeros((1, COLS), f32)

        tiles(0, POINTS[1], clear)

        def clear2(p):
            sc["g2"][p, 0] = zero

        tiles(0, POINTS[2], clear2)

    def no_bottom():
        def clear(p):
            sc["hb"][p] = jnp.zeros((1, COLS), f32)

        tiles(0, POINTS[1], clear)

        def clear2(p):
            sc["g2"][p, 2] = zero

        tiles(0, POINTS[2], clear2)

    when(b + s == 0, no_top)
    when(b + s == TILES + STRIPS - 2, no_bottom)

    for load in loads:
        load.wait()

    def damp(i):
        e = 0.8 / (1.0 + 4.0 * de[i])
        ee[i] = e
        wo[i] = e * ge[1, i]

    def sweep_a(i):
        va[i] = 0.2 * ge[0, i] + ee[i] * (fe[0, i] + de[i] * around(ge.at[0], i))

    def sweep_b(i):
        vb[i] = 0.2 * ge[1, i] + ee[i] * (fe[1, i] + de[i] * around(ge.at[1], i) + ge[0, i])

    def give(i):
        uo[i] = (vb[i] - 0.8 * ge[1, i]) + (de[i] * around(wo, i) + wo[i])

    def resid0(i):
        d = de[i]
        diag = 1.0 + 4.0 * d
        a, bb = va[i], vb[i]
        ra[i] = (fe[0, i] - diag * a) + d * around(va, i)
        rb[i] = (fe[1, i] - diag * bb) + (d * around(vb, i) + a)

    spans = ((3, 7), (10, 7), (17, 7), (24, 7), (1, 2), (31, 2), (0, 1), (EXT - 1, 1))
    give_copies = []
    for k, (lo, n) in enumerate(spans):
        at = pl.ds(lo, n)
        give_copies.append(remote(uo.at[at], ui.at[at], sc["us"].at[k], sc["ur"].at[k], next_id))

    def inner_span(k):
        lo, n = spans[k]
        end = lo + n + (k == 3)
        tiles(1 if k == 0 else lo + 1, end + 1, damp)
        tiles(2 if k == 0 else lo, end, sweep_b)
        tiles(lo, lo + n, give)

    inner_span(0)

    peers = GROUP - 1 + HALVES * STRIPS - 1 + 1
    extra = (h == 0) & (j > 0)
    when(extra, lambda: pl.semaphore_wait(barrier, peers + 1))
    when(jnp.logical_not(extra), lambda: pl.semaphore_wait(barrier, peers))

    halo = []
    for k, ref in enumerate((ge.at[1], de, ge.at[0], fe.at[0], fe.at[1])):
        halo.append((
            remote(ref.at[1], ref.at[EXT - 1], sc["hs"].at[k, 0], sc["hr"].at[k, 0], north_id),
            remote(ref.at[TILES], ref.at[0], sc["hs"].at[k, 1], sc["hr"].at[k, 1], south_id),
        ))
    for north, south in halo:
        when(s > 0, north.start)
        when(s < STRIPS - 1, south.start)
    when(has_next, give_copies[0].start)
    for k in range(1, 4):
        inner_span(k)
        when(has_next, give_copies[k].start)
    tiles(2, TILES, sweep_a)
    tiles(3, TILES - 1, resid0)

    def land_halo(pairs):
        for north, south in pairs:
            when(s > 0, north.wait_send)
            when(s < STRIPS - 1, north.wait_recv)
            when(s < STRIPS - 1, south.wait_send)
            when(s > 0, south.wait_recv)

    land_halo(halo[:2])
    damp(0)
    damp(EXT - 1)

    def no_row(at):
        ee[at] = zero
        wo[at] = zero

    when(s == 0, lambda: no_row(0))
    when(s == STRIPS - 1, lambda: no_row(EXT - 1))
    sweep_b(1)
    sweep_b(TILES)
    tiles(1, 3, give)
    when(has_next, give_copies[4].start)
    tiles(TILES - 1, TILES + 1, give)
    when(has_next, give_copies[5].start)
    land_halo(halo[2:])
    for i in (0, EXT - 1):
        sweep_b(i)
        sweep_a(i)
        give(i)
    when(has_next, give_copies[6].start)
    when(has_next, give_copies[7].start)
    sweep_a(1)
    sweep_a(TILES)

    g1, go = sc["g1"], sc["go"]
    tiles(1, 3, resid0)
    tiles(TILES - 1, TILES + 1, resid0)

    def scatter(i):
        g = (ra[i] + rb[i]) + ui[i]
        go[i - 1] = g
        rank = rank_of(i - 1)

        def keep():
            g1[j] = g

        when(rank == j, keep)
        copy = remote(go.at[i - 1], g1.at[j], sc["gs"], sc["gr"], (h * GROUP + rank, s))
        when(rank != j, copy.start)

    for copy, (lo, n) in zip(give_copies[:6], spans):
        when(has_prev, copy.wait_recv)

        def turn(r, lo=lo, n=n):
            scatter(lo + (b + r) % n)

        tiles(0, n, turn)

    even = m % 2 == 0
    wi = sc["wi"]
    parts = ((0, 9), (9, 9), (18, 8), (26, 8))
    p_copies = []
    x_copies = []
    for k, (lo, n) in enumerate(parts):
        at = pl.ds(lo, n)
        p_copies.append(remote(ge.at[1, at], pe.at[at], sc["ps"].at[k], sc["pr"].at[k], next_id))
        x_copies.append(remote(xo.at[at], xi.at[at], sc["qs"].at[k], sc["qr"].at[k], next_id))

    def complete(i):
        w = ee[i] * pe[i]
        va[i] = va[i] + w
        wi[i] = w

    def hand_on(i):
        xo[i] = 0.2 * vb[i] + ee[i] * (fe[1, i] + de[i] * around(vb, i) + va[i])

    def level0_again():
        for copy in p_copies:
            when(has_prev, copy.wait_recv)
        tiles(0, EXT, complete)
        tiles(0, EXT, hand_on)

    def start_p():
        for copy in p_copies:
            copy.start()

    when(even, start_p)
    odd_one = jnp.logical_not(even)
    when(odd_one, level0_again)
    far_next = odd_one & has_next

    em, sm = sc["em"], sc["sm"]
    for t in range(3):
        d = de[b + t]
        for level in range(1, 5):
            em[level - 1, t] = 0.8 / (1.0 + 4.0 * (2.0**level * d))
            sm[level - 1, t] = 2.0**level * d

    def no_damp(t):
        for level in range(1, 5):
            em[level - 1, t] = zero

    when(b + s == 0, lambda: no_damp(0))
    when(b + s == TILES + STRIPS - 2, lambda: no_damp(2))
    all_in = remote(go.at[pl.ds(0, GROUP - 1)], g1.at[pl.ds(0, GROUP - 1)], sc["gs"], sc["gr"], next_id)
    all_in.wait_recv()

    g2, g3, g4 = sc["g2"], sc["g3"], sc["g4"]
    v1, v2, v3, v4a, v4b = sc["v1"], sc["v2"], sc["v3"], sc["v4a"], sc["v4b"]
    n2, n3, ht, hb = sc["n2"], sc["n3"], sc["ht"], sc["hb"]
    halves = []

    def to_half(ref, count):
        k = len(halves)
        copy = remote(ref.at[count], ref.at[0], sc["xs"].at[k], sc["xr"].at[k], half_id)
        halves.append(copy)
        when(h == 0, copy.start)
        return copy

    def first_sweep(p):
        v = em[0, 1] * g1[p]
        v1[p + 1] = v
        sc["st"][p] = v[0:1]
        sc["sb"][p] = v[7:8]

    tiles(0, POINTS[1], first_sweep)
    sides = [
        (has_up, has_dn, remote(sc["st"], hb, sc["ys"].at[0], sc["yr"].at[0], up_id)),
        (has_dn, has_up, remote(sc["sb"], ht, sc["ys"].at[1], sc["yr"].at[1], dn_id)),
    ]

    def start(copies):
        for sends, _, copy in copies:
            when(sends, copy.start)

    def land(copies):
        for _, takes, copy in copies:
            when(takes, copy.wait_recv)

    start(sides)
    copy = to_half(v1, POINTS[1])
    land(sides)
    when(h == 1, copy.wait_recv)

    def descend1(q, acc):
        scaled = sm[0, 1]
        p = 2 * q
        before, now, after = v1[p], v1[p + 1], v1[p + 2]
        r0 = (0.2 * g1[p] + scaled * nb(now, ht[p], hb[p])) + before
        r1 = (0.2 * g1[p + 1] + scaled * nb(after, ht[p + 1], hb[p + 1])) + now
        g2[q, 1] = r0 + r1
        return acc + (r0 * r0 + r1 * r1)

    sc["acc"][1] = lax.fori_loop(0, POINTS[2], descend1, zero)
    mine2 = g2.at[:, 1]
    wide = [
        (has_up, has_dn, remote(mine2, g2.at[:, 2], sc["ys"].at[2], sc["yr"].at[2], up_id)),
        (has_dn, has_up, remote(mine2, g2.at[:, 0], sc["ys"].at[3], sc["yr"].at[3], dn_id)),
    ]
    start(wide)
    for part in p_copies + x_copies:
        when(far_next, part.start)
    land(wide)

    def around3(parts, t):
        return nb(parts[t], parts[max(t - 1, 0)], parts[min(t + 1, 2)])

    def sweep2(p):
        for t in range(3):
            v2[p + 1, t] = em[1, t] * g2[p, t]

    tiles(0, POINTS[2], sweep2)
    copy = to_half(v2, POINTS[2])
    when(h == 1, copy.wait_recv)

    for level, v, g, coarse, vc in ((2, v2, g2, g3, v3), (3, v3, g3, g4, v4a)):
        def descend(q, acc, level=level, v=v, g=g, coarse=coarse, vc=vc):
            p = 2 * q
            now = [v[p + 1, t] for t in range(3)]
            after = [v[p + 2, t] for t in range(3)]
            for t in range(3):
                scaled = sm[level - 1, t]
                r0 = (0.2 * g[p, t] + scaled * around3(now, t)) + v[p, t]
                r1 = (0.2 * g[p + 1, t] + scaled * around3(after, t)) + now[t]
                total = r0 + r1
                coarse[q, t] = total
                vc[q + 1, t] = em[level, t] * total
                if t == 1:
                    acc = acc + (r0 * r0 + r1 * r1)
            return acc

        sc["acc"][level] = lax.fori_loop(0, POINTS[level + 1], descend, zero)
        copy = to_half(vc, POINTS[level + 1])
        when(h == 1, copy.wait_recv)
    def second_sweep(p):
        now = [v4a[p + 1, t] for t in range(3)]
        for t in range(3):
            v4b[p + 1, t] = 0.2 * now[t] + em[3, t] * (
                g4[p, t] + sm[3, t] * around3(now, t) + v4a[p, t]
            )

    tiles(0, POINTS[4], second_sweep)
    copy = to_half(v4b, POINTS[4])
    when(h == 1, copy.wait_recv)

    def last_resid(p, acc):
        now = [v4b[p + 1, t] for t in range(3)]
        scaled = sm[3, 1]
        r = (g4[p, 1] - (1.0 + 4.0 * scaled) * now[1]) + (scaled * around3(now, 1) + v4b[p, 1])
        return acc + r * r

    sc["acc"][4] = lax.fori_loop(0, POINTS[4], last_resid, zero)

    for level, v, g, c, new in ((3, v3, g3, v4b, n3), (2, v2, g2, n3, n2)):
        def ascend(q, level=level, v=v, g=g, c=c, new=new):
            this = [c[q + 1, t] for t in range(3)]
            before = [v[2 * q, t] + c[q, t] for t in range(3)]
            for i in range(2):
                p = 2 * q + i
                now = [v[p + 1, t] + this[t] for t in range(3)]
                for t in range(3):
                    new[p + 1, t] = 0.2 * now[t] + em[level - 1, t] * (
                        g[p, t] + sm[level - 1, t] * around3(now, t) + before[t]
                    )
                before = now

        tiles(0, POINTS[level] // 2, ascend)
        copy = to_half(new, POINTS[level])
        when(h == 1, copy.wait_recv)
    no = sc["no"]

    def ascend1(q):
        scaled, e = sm[0, 1], em[0, 1]
        this, top, bottom = n2[q + 1, 1], n2[q + 1, 0], n2[q + 1, 2]
        before = v1[2 * q] + n2[q, 1]
        for i in range(2):
            p = 2 * q + i
            now = v1[p + 1] + this
            around_it = nb(now, ht[p] + top, hb[p] + bottom)
            no[p] = 0.2 * now + e * (g1[p] + scaled * around_it + before)
            before = now

    tiles(0, POINTS[1] // 2, ascend1)

    def back(r):
        p = (r + GROUP - b) % GROUP
        after = h * GROUP + p + 1
        tile = b + 1

        def keep():
            n1[tile] = no[p]

        def keep_prev():
            np_[tile] = no[p]

        copy = remote(no.at[p], n1.at[tile], sc["bs"], sc["br"].at[b], (h * GROUP + p, s))
        when(p == j, keep)
        when(p != j, copy.start)
        ahead = remote(no.at[p], np_.at[tile], sc["cs"], sc["fr"], (after % (GROUP * HALVES), s))
        crosses = (p % 2 == 1) & (after < GROUP * HALVES)
        when(crosses & (after == m), keep_prev)
        when(crosses & (after != m), ahead.start)

    tiles(0, GROUP, back)

    when(even, level0_again)

    def start_x():
        for copy in x_copies:
            copy.start()

    when(even, start_x)
    for copy in give_copies[6:]:
        when(has_prev, copy.wait_recv)

    def carry_over(i):
        vp[i] = ((ui[i] - wi[i]) + 0.8 * pe[i]) - de[i] * around(wi, i)

    tiles(0, EXT, carry_over)

    def energy(i, acc):
        r0 = ra[i] + (ui[i] - wi[i])
        r1 = rb[i] + wi[i]
        return acc + (r0 * r0 + r1 * r1)

    sc["acc"][0] = lax.fori_loop(1, TILES + 1, energy, zero)

    def forward(tile):
        return remote(n1.at[tile], np_.at[tile], sc["fs"], sc["fr"], next_id)

    edge_north = remote(n1.at[1], n1.at[EXT - 1], sc["es"].at[0], sc["er"].at[0], north_id)
    edge_south = remote(n1.at[TILES], n1.at[0], sc["es"].at[1], sc["er"].at[1], south_id)

    def correct(i):
        t = n1[i]
        va[i] = va[i] + t
        vb[i] = vb[i] + t

    def arrive(r):
        i = (r + GROUP - j) % GROUP
        copy = remote(n1.at[i + 1], n1.at[i + 1], sc["bs"], sc["br"].at[i], next_id)
        when(i != b, copy.wait_recv)
        when(even, forward(i + 1).start)
        when((i == 0) & (s > 0), edge_north.start)
        when((i == TILES - 1) & (s < STRIPS - 1), edge_south.start)
        correct(i + 1)

    tiles(0, TILES, arrive)
    when(s < STRIPS - 1, edge_north.wait_recv)
    when(s > 0, edge_south.wait_recv)
    when(has_next, forward(0).start)
    when(has_next, forward(EXT - 1).start)
    correct(0)
    correct(EXT - 1)

    for copy in x_copies:
        when(has_prev, copy.wait_recv)
    def some(n, name):
        at = pl.ds(0, n)
        return remote(n1.at[at], np_.at[at], sc[name], sc["fr"], next_id)

    inside = even & (j > 0)
    when(has_prev & jnp.logical_not(inside), some(EXT, "fs").wait_recv)
    when(inside, some(EXT - 1, "fs").wait_recv)

    def last_sweep(i):
        e, d = ee[i], de[i]
        a, bb = va[i], vb[i]
        ra[i] = 0.2 * a + e * (fe[0, i] + d * around(va, i) + (vp[i] + np_[i]))
        rb[i] = 0.2 * bb + e * (fe[1, i] + d * around(vb, i) + a)

    tiles(0, EXT, last_sweep)
    writes = [
        pltpu.make_async_copy(ra.at[inner], out.at[0], sc["write"].at[0]),
        pltpu.make_async_copy(rb.at[inner], out.at[1], sc["write"].at[1]),
    ]
    for write in writes:
        write.start()

    def final(i, acc):
        e, d = ee[i], de[i]
        diag = 1.0 + 4.0 * d
        a, bb, t = ra[i], rb[i], np_[i]
        before = xi[i] + (0.2 * t + e * (d * around(np_, i) + t))
        r0 = (fe[0, i] - diag * a) + (d * around(ra, i) + before)
        r1 = (fe[1, i] - diag * bb) + (d * around(rb, i) + a)
        return acc + (r0 * r0 + r1 * r1)

    sc["acc"][5] = lax.fori_loop(1, TILES + 1, final, zero)

    lines = lax.broadcasted_iota(jnp.int32, (8, 128), 0)
    part = jnp.zeros((8, 128), f32)
    for k in range(6):
        whole_sum = sc["acc"][k]
        narrow = whole_sum[:, 0:128]
        for c in range(1, COLS // 128):
            narrow = narrow + whole_sum[:, c * 128:(c + 1) * 128]
        part = jnp.where(lines == k, jnp.sum(narrow, axis=0, keepdims=True), part)
    sc["t0"][...] = part
    sc["q0"][j] = part

    def tell(r, carry):
        copy = remote(sc["t0"], sc["q0"].at[j], sc["ns"].at[0], sc["nr"].at[0], (h * GROUP + (j + r) % GROUP, s))
        copy.start()
        return carry

    lax.fori_loop(1, GROUP, tell, 0)
    heard = remote(sc["q0"].at[pl.ds(0, GROUP - 1)], sc["q0"].at[pl.ds(0, GROUP - 1)], sc["ns"].at[0], sc["nr"].at[0], next_id)
    heard.wait_recv()
    part = sc["q0"][0]
    for k in range(1, GROUP):
        part = part + sc["q0"][k]
    sc["t1"][...] = part
    sc["q1"][mine] = part

    def tell_far(r, carry):
        other = (mine + r) % (HALVES * STRIPS)
        device = ((other // STRIPS) * GROUP + j, other % STRIPS)
        remote(sc["t1"], sc["q1"].at[mine], sc["ns"].at[1], sc["nr"].at[1], device).start()
        return carry

    lax.fori_loop(1, HALVES * STRIPS, tell_far, 0)
    far = pl.ds(0, HALVES * STRIPS - 1)
    heard_far = remote(sc["q1"].at[far], sc["q1"].at[far], sc["ns"].at[1], sc["nr"].at[1], next_id)
    heard_far.wait_recv()
    part = sc["q1"][0]
    for k in range(1, HALVES * STRIPS):
        part = part + sc["q1"][k]
    total = jnp.sum(part, axis=1, keepdims=True)
    norms[...] = jnp.broadcast_to(jnp.sqrt(total / CELLS), (8, 128))

    for copy in give_copies + p_copies + x_copies:
        when(has_next, copy.wait_send)
    for sends, _, copy in sides + wide:
        when(sends, copy.wait_send)
    for copy in halves:
        when(h == 0, copy.wait_send)
    all_in.wait_send()
    remote(no.at[pl.ds(0, GROUP - 1)], no.at[pl.ds(0, GROUP - 1)], sc["bs"], sc["br"].at[0], next_id).wait_send()
    when(even, some(EXT, "fs").wait_send)
    when(has_next & jnp.logical_not(even), some(2, "fs").wait_send)
    for half in range(HALVES):
        when((h == half) & inside, some(GROUP // 2 - 1 - half, "cs").wait_send)
        when((h == half) & jnp.logical_not(inside), some(GROUP // 2 - half, "cs").wait_send)
    when(s > 0, edge_north.wait_send)
    when(s < STRIPS - 1, edge_south.wait_send)
    heard.wait_send()
    heard_far.wait_send()
    for write in writes:
        write.wait()


def scratch():
    ext = pltpu.VMEM((EXT, 8, COLS), f32)
    shapes = {"fe": pltpu.VMEM((2, EXT, 8, COLS), f32), "ge": pltpu.VMEM((2, EXT, 8, COLS), f32)}
    for name in ("de", "ee", "va", "vb", "ra", "rb", "uo", "ui", "pe", "xo", "xi", "vp", "wo", "wi", "n1", "np"):
        shapes[name] = ext
    for name in ("g1", "go", "no"):
        shapes[name] = pltpu.VMEM((GROUP, 8, COLS), f32)
    for name, level in (("g2", 2), ("g3", 3), ("g4", 4)):
        shapes[name] = pltpu.VMEM((POINTS[level], 3, 8, COLS), f32)
    shapes["v1"] = pltpu.VMEM((POINTS[1] + 1, 8, COLS), f32)
    for name, level in (("v2", 2), ("v3", 3), ("v4a", 4), ("v4b", 4), ("n3", 3), ("n2", 2)):
        shapes[name] = pltpu.VMEM((POINTS[level] + 1, 3, 8, COLS), f32)
    for name in ("st", "sb", "ht", "hb"):
        shapes[name] = pltpu.VMEM((POINTS[1], 1, COLS), f32)
    shapes["em"] = shapes["sm"] = pltpu.VMEM((4, 3, 8, COLS), f32)
    shapes["acc"] = pltpu.VMEM((6, 8, COLS), f32)
    shapes["t0"] = shapes["t1"] = pltpu.VMEM((8, 128), f32)
    shapes["q0"] = pltpu.VMEM((GROUP, 8, 128), f32)
    shapes["q1"] = pltpu.VMEM((HALVES * STRIPS, 8, 128), f32)
    for name, dims in (
        ("load", (4,)), ("hs", (5, 2)), ("hr", (5, 2)), ("us", (8,)), ("ur", (8,)),
        ("gs", ()), ("gr", ()), ("xs", (7,)), ("xr", (7,)), ("ys", (4,)), ("yr", (4,)), ("cs", ()), ("ps", (4,)), ("pr", (4,)),
        ("qs", (4,)), ("qr", (4,)), ("bs", ()), ("br", (TILES,)), ("fs", ()), ("fr", ()),
        ("es", (2,)), ("er", (2,)), ("ns", (2,)), ("nr", (2,)), ("write", (2,)),
    ):
        shapes[name] = pltpu.SemaphoreType.DMA(dims)
    return shapes


def body(rhs, guess, diffusion):
    anywhere = pl.BlockSpec(memory_space=pl.ANY)
    field, norms = pl.pallas_call(
        kernel,
        out_shape=(
            jax.ShapeDtypeStruct((2, TILES, 8, COLS), f32),
            jax.ShapeDtypeStruct((8, 128), f32),
        ),
        in_specs=[anywhere] * 3,
        out_specs=(anywhere, pl.BlockSpec(memory_space=pltpu.VMEM)),
        scratch_shapes=[scratch()],
        compiler_params=pltpu.CompilerParams(collective_id=0, has_side_effects=True, vmem_limit_bytes=60000 * 1024),
        name="cycle",
    )(
        rhs.reshape(2, TILES, 8, COLS),
        guess.reshape(2, TILES, 8, COLS),
        diffusion.reshape(TILES, 8, COLS),
    )
    return field.reshape(2, TILES * 8, COLS), norms[:6, 0]


def solution(mesh):
    return jax.shard_map(
        body,
        mesh=mesh,
        in_specs=(P("tm", "space", None), P("tm", "space", None), P("space", None)),
        out_specs=(P("tm", "space", None), P()),
        check_vma=False,
    )
```

```python
import jax
import jax.numpy as jnp
from jax import lax
from jax.experimental import pallas as pl
from jax.experimental.pallas import tpu as pltpu
from jax.sharding import PartitionSpec as P

MESH = pl.DeviceIdType.MESH
f32 = jnp.float32
GROUP = 32
HALVES = 2
STRIPS = 4
TILES = 32
EXT = TILES + 2
COLS = 1024
CELLS = 1048576.0
POINTS = {1: 32, 2: 16, 3: 8, 4: 4}


def snake(j):
    y = j // 8
    x = (j // 2 + 2) % 4
    x = x + (y % 2) * (3 - 2 * x)
    return (y * 4 + x) * 2 + j % 2


def kernel(rhs, guess, diff, out, norms, sc):
    m = lax.axis_index("tm")
    s = lax.axis_index("space")
    j = m % GROUP
    h = m // GROUP
    odd = s % 2

    def mirror(j, h):
        return j + h * 8 * (3 - 2 * (j // 8))

    def rank_of(b, h=h):
        return mirror(snake(b + odd * (TILES - 1 - 2 * b)), h)

    place = snake(mirror(j, h))
    b = place + odd * (TILES - 1 - 2 * place)
    first = (TILES - 1 - b) // (TILES - 1)
    last = b // (TILES - 1)
    up_id = (h * GROUP + rank_of(b - 1 + first), (s - first + STRIPS) % STRIPS)
    dn_id = (h * GROUP + rank_of(b + 1 - last), (s + last) % STRIPS)
    has_up = b + s > 0
    has_dn = b + s < TILES + STRIPS - 2
    next_id = ((m + 1) % (GROUP * HALVES), s)
    half_id = ((1 - h) * GROUP + rank_of(b, 1 - h), s)
    north_id = (m, (s + STRIPS - 1) % STRIPS)
    south_id = (m, (s + 1) % STRIPS)
    has_next = m < GROUP * HALVES - 1
    has_prev = m > 0

    row = lax.broadcasted_iota(jnp.int32, (8, COLS), 0)
    col = lax.broadcasted_iota(jnp.int32, (8, COLS), 1)

    def nb(tile, above, below):
        up = pltpu.roll(jnp.where(row == 7, above, tile), 1, 0)
        down = pltpu.roll(jnp.where(row == 0, below, tile), 7, 0)
        left = jnp.where(col == 0, 0.0, pltpu.roll(tile, 1, 1))
        right = jnp.where(col == COLS - 1, 0.0, pltpu.roll(tile, COLS - 1, 1))
        return (up + down) + (left + right)

    def around(ref, i):
        return nb(ref[i], ref[i - 1 + (EXT - 1 - i) // (EXT - 1)], ref[i + 1 - i // (EXT - 1)])

    def tiles(lo, hi, fn):
        def step(i, carry):
            fn(i)
            return carry

        lax.fori_loop(lo, hi, step, 0)

    def remote(src, dst, send, recv, device):
        return pltpu.make_async_remote_copy(
            src_ref=src, dst_ref=dst, send_sem=send, recv_sem=recv,
            device_id=device, device_id_type=MESH,
        )

    def when(cond, fn):
        pl.when(cond)(fn)

    fe, ge, de, ee = sc["fe"], sc["ge"], sc["de"], sc["ee"]
    va, vb, ra, rb = sc["va"], sc["vb"], sc["ra"], sc["rb"]
    uo, ui, pe, xo, xi, vp = sc["uo"], sc["ui"], sc["pe"], sc["xo"], sc["xi"], sc["vp"]
    wo, n1, np_ = sc["wo"], sc["n1"], sc["np"]

    inner = pl.ds(1, TILES)
    loads = [
        pltpu.make_async_copy(guess.at[1], ge.at[1, inner], sc["load"].at[0]),
        pltpu.make_async_copy(diff, de.at[inner], sc["load"].at[1]),
        pltpu.make_async_copy(guess.at[0], ge.at[0, inner], sc["load"].at[2]),
        pltpu.make_async_copy(rhs, fe.at[:, inner], sc["load"].at[3]),
    ]
    for load in loads:
        load.start()

    barrier = pltpu.get_barrier_semaphore()

    def greet(device):
        pl.semaphore_signal(barrier, inc=1, device_id=device, device_id_type=MESH)

    def greet_rank(r, carry):
        greet((h * GROUP + (j + r) % GROUP, s))
        return carry

    lax.fori_loop(1, GROUP, greet_rank, 0)
    mine = h * STRIPS + s

    def greet_other(r, carry):
        other = (mine + r) % (HALVES * STRIPS)
        greet(((other // STRIPS) * GROUP + j, other % STRIPS))
        return carry

    lax.fori_loop(1, HALVES * STRIPS, greet_other, 0)
    greet(half_id)
    def greet_first_half():
        def greet_one(r, carry):
            greet((r, s))
            return carry

        lax.fori_loop(1, GROUP, greet_one, 0)

    when(m == GROUP, greet_first_half)

    zero = jnp.zeros((8, COLS), f32)

    def outside(at):
        for ref in (ge.at[1], de, ge.at[0], fe.at[0], fe.at[1], n1):
            ref[at] = zero

    when(s == 0, lambda: outside(0))
    when(s == STRIPS - 1, lambda: outside(EXT - 1))

    def no_prev():
        def clear(i):
            for ref in (ui, pe, xi, np_):
                ref[i] = zero

        tiles(0, EXT, clear)

    when(m == 0, no_prev)

    def no_half():
        sc["v1"][0] = zero
        for name in ("v2", "v3", "v4a", "v4b", "n3", "n2"):
            for t in range(3):
                sc[name][0, t] = zero

    when(h == 0, no_half)

    def no_top():
        def clear(p):
            sc["ht"][p] = jnp.zeros((1, COLS), f32)

        tiles(0, POINTS[1], clear)

        def clear2(p):
            sc["g2"][p, 0] = zero

        tiles(0, POINTS[2], clear2)

    def no_bottom():
        def clear(p):
            sc["hb"][p] = jnp.zeros((1, COLS), f32)

        tiles(0, POINTS[1], clear)

        def clear2(p):
            sc["g2"][p, 2] = zero

        tiles(0, POINTS[2], clear2)

    when(b + s == 0, no_top)
    when(b + s == TILES + STRIPS - 2, no_bottom)

    for load in loads:
        load.wait()

    def damp(i):
        e = 0.8 / (1.0 + 4.0 * de[i])
        ee[i] = e
        wo[i] = e * ge[1, i]

    def sweep_a(i):
        va[i] = 0.2 * ge[0, i] + ee[i] * (fe[0, i] + de[i] * around(ge.at[0], i))

    def sweep_b(i):
        vb[i] = 0.2 * ge[1, i] + ee[i] * (fe[1, i] + de[i] * around(ge.at[1], i) + ge[0, i])

    def give(i):
        uo[i] = (vb[i] - 0.8 * ge[1, i]) + (de[i] * around(wo, i) + wo[i])

    def resid0(i):
        d = de[i]
        diag = 1.0 + 4.0 * d
        a, bb = va[i], vb[i]
        ra[i] = (fe[0, i] - diag * a) + d * around(va, i)
        rb[i] = (fe[1, i] - diag * bb) + (d * around(vb, i) + a)

    spans = ((3, 7), (10, 7), (17, 7), (24, 7), (1, 2), (31, 2), (0, 1), (EXT - 1, 1))
    give_copies = []
    for k, (lo, n) in enumerate(spans):
        at = pl.ds(lo, n)
        give_copies.append(remote(uo.at[at], ui.at[at], sc["us"].at[k], sc["ur"].at[k], next_id))

    def inner_span(k):
        lo, n = spans[k]
        end = lo + n + (k == 3)
        tiles(1 if k == 0 else lo + 1, end + 1, damp)
        tiles(2 if k == 0 else lo, end, sweep_b)
        tiles(lo, lo + n, give)

    inner_span(0)

    peers = GROUP - 1 + HALVES * STRIPS - 1 + 1
    extra = (h == 0) & (j > 0)
    when(extra, lambda: pl.semaphore_wait(barrier, peers + 1))
    when(jnp.logical_not(extra), lambda: pl.semaphore_wait(barrier, peers))

    halo = []
    for k, ref in enumerate((ge.at[1], de, ge.at[0], fe.at[0], fe.at[1])):
        halo.append((
            remote(ref.at[1], ref.at[EXT - 1], sc["hs"].at[k, 0], sc["hr"].at[k, 0], north_id),
            remote(ref.at[TILES], ref.at[0], sc["hs"].at[k, 1], sc["hr"].at[k, 1], south_id),
        ))
    for north, south in halo:
        when(s > 0, north.start)
        when(s < STRIPS - 1, south.start)
    when(has_next, give_copies[0].start)
    for k in range(1, 4):
        inner_span(k)
        when(has_next, give_copies[k].start)
    tiles(2, TILES, sweep_a)
    tiles(3, TILES - 1, resid0)

    def land_halo(pairs):
        for north, south in pairs:
            when(s > 0, north.wait_send)
            when(s < STRIPS - 1, north.wait_recv)
            when(s < STRIPS - 1, south.wait_send)
            when(s > 0, south.wait_recv)

    land_halo(halo[:2])
    damp(0)
    damp(EXT - 1)

    def no_row(at):
        ee[at] = zero
        wo[at] = zero

    when(s == 0, lambda: no_row(0))
    when(s == STRIPS - 1, lambda: no_row(EXT - 1))
    sweep_b(1)
    sweep_b(TILES)
    tiles(1, 3, give)
    when(has_next, give_copies[4].start)
    tiles(TILES - 1, TILES + 1, give)
    when(has_next, give_copies[5].start)
    land_halo(halo[2:])
    for i in (0, EXT - 1):
        sweep_b(i)
        sweep_a(i)
        give(i)
    when(has_next, give_copies[6].start)
    when(has_next, give_copies[7].start)
    sweep_a(1)
    sweep_a(TILES)

    g1, go = sc["g1"], sc["go"]
    tiles(1, 3, resid0)
    tiles(TILES - 1, TILES + 1, resid0)

    def scatter(i):
        g = (ra[i] + rb[i]) + ui[i]
        go[i - 1] = g
        rank = rank_of(i - 1)

        def keep():
            g1[j] = g

        when(rank == j, keep)
        copy = remote(go.at[i - 1], g1.at[j], sc["gs"], sc["gr"], (h * GROUP + rank, s))
        when(rank != j, copy.start)

    for copy, (lo, n) in zip(give_copies[:6], spans):
        when(has_prev, copy.wait_recv)

        def turn(r, lo=lo, n=n):
            scatter(lo + (b + r) % n)

        tiles(0, n, turn)

    even = m % 2 == 0
    wi = sc["wi"]
    parts = ((0, 9), (9, 9), (18, 8), (26, 8))
    p_copies = []
    x_copies = []
    for k, (lo, n) in enumerate(parts):
        at = pl.ds(lo, n)
        p_copies.append(remote(ge.at[1, at], pe.at[at], sc["ps"].at[k], sc["pr"].at[k], next_id))
        x_copies.append(remote(xo.at[at], xi.at[at], sc["qs"].at[k], sc["qr"].at[k], next_id))

    def complete(i):
        w = ee[i] * pe[i]
        va[i] = va[i] + w
        wi[i] = w

    def hand_on(i):
        xo[i] = 0.2 * vb[i] + ee[i] * (fe[1, i] + de[i] * around(vb, i) + va[i])

    def level0_again():
        for copy in p_copies:
            when(has_prev, copy.wait_recv)
        tiles(0, EXT, complete)
        tiles(0, EXT, hand_on)

    def start_p():
        for copy in p_copies:
            copy.start()

    when(even, start_p)
    odd_one = jnp.logical_not(even)
    when(odd_one, level0_again)
    far_next = odd_one & has_next

    em, sm = sc["em"], sc["sm"]
    for t in range(3):
        d = de[b + t]
        for level in range(1, 5):
            em[level - 1, t] = 0.8 / (1.0 + 4.0 * (2.0**level * d))
            sm[level - 1, t] = 2.0**level * d

    def no_damp(t):
        for level in range(1, 5):
            em[level - 1, t] = zero

    when(b + s == 0, lambda: no_damp(0))
    when(b + s == TILES + STRIPS - 2, lambda: no_damp(2))
    all_in = remote(go.at[pl.ds(0, GROUP - 1)], g1.at[pl.ds(0, GROUP - 1)], sc["gs"], sc["gr"], next_id)
    all_in.wait_recv()

    g2, g3, g4 = sc["g2"], sc["g3"], sc["g4"]
    v1, v2, v3, v4a, v4b = sc["v1"], sc["v2"], sc["v3"], sc["v4a"], sc["v4b"]
    n2, n3, ht, hb = sc["n2"], sc["n3"], sc["ht"], sc["hb"]
    halves = []

    def to_half(ref, count):
        k = len(halves)
        copy = remote(ref.at[count], ref.at[0], sc["xs"].at[k], sc["xr"].at[k], half_id)
        halves.append(copy)
        when(h == 0, copy.start)
        return copy

    def first_sweep(p):
        v = em[0, 1] * g1[p]
        v1[p + 1] = v
        sc["st"][p] = v[0:1]
        sc["sb"][p] = v[7:8]

    tiles(0, POINTS[1], first_sweep)
    sides = [
        (has_up, has_dn, remote(sc["st"], hb, sc["ys"].at[0], sc["yr"].at[0], up_id)),
        (has_dn, has_up, remote(sc["sb"], ht, sc["ys"].at[1], sc["yr"].at[1], dn_id)),
    ]

    def start(copies):
        for sends, _, copy in copies:
            when(sends, copy.start)

    def land(copies):
        for _, takes, copy in copies:
            when(takes, copy.wait_recv)

    start(sides)
    copy = to_half(v1, POINTS[1])
    land(sides)
    when(h == 1, copy.wait_recv)

    def descend1(q, acc):
        scaled = sm[0, 1]
        p = 2 * q
        before, now, after = v1[p], v1[p + 1], v1[p + 2]
        r0 = (0.2 * g1[p] + scaled * nb(now, ht[p], hb[p])) + before
        r1 = (0.2 * g1[p + 1] + scaled * nb(after, ht[p + 1], hb[p + 1])) + now
        g2[q, 1] = r0 + r1
        return acc + (r0 * r0 + r1 * r1)

    sc["acc"][1] = lax.fori_loop(0, POINTS[2], descend1, zero)
    mine2 = g2.at[:, 1]
    wide = [
        (has_up, has_dn, remote(mine2, g2.at[:, 2], sc["ys"].at[2], sc["yr"].at[2], up_id)),
        (has_dn, has_up, remote(mine2, g2.at[:, 0], sc["ys"].at[3], sc["yr"].at[3], dn_id)),
    ]
    start(wide)
    for part in p_copies[:2]:
        when(far_next, part.start)
    for part in p_copies[2:] + x_copies[:2]:
        when(far_next & (h == 1), part.start)
    land(wide)

    def around3(parts, t):
        return nb(parts[t], parts[max(t - 1, 0)], parts[min(t + 1, 2)])

    def sweep2(p):
        for t in range(3):
            v2[p + 1, t] = em[1, t] * g2[p, t]

    tiles(0, POINTS[2], sweep2)
    copy = to_half(v2, POINTS[2])
    when(h == 1, copy.wait_recv)

    for level, v, g, coarse, vc in ((2, v2, g2, g3, v3), (3, v3, g3, g4, v4a)):
        def descend(q, acc, level=level, v=v, g=g, coarse=coarse, vc=vc):
            p = 2 * q
            now = [v[p + 1, t] for t in range(3)]
            after = [v[p + 2, t] for t in range(3)]
            for t in range(3):
                scaled = sm[level - 1, t]
                r0 = (0.2 * g[p, t] + scaled * around3(now, t)) + v[p, t]
                r1 = (0.2 * g[p + 1, t] + scaled * around3(after, t)) + now[t]
                total = r0 + r1
                coarse[q, t] = total
                vc[q + 1, t] = em[level, t] * total
                if t == 1:
                    acc = acc + (r0 * r0 + r1 * r1)
            return acc

        sc["acc"][level] = lax.fori_loop(0, POINTS[level + 1], descend, zero)
        copy = to_half(vc, POINTS[level + 1])
        when(h == 1, copy.wait_recv)
    def second_sweep(p):
        now = [v4a[p + 1, t] for t in range(3)]
        for t in range(3):
            v4b[p + 1, t] = 0.2 * now[t] + em[3, t] * (
                g4[p, t] + sm[3, t] * around3(now, t) + v4a[p, t]
            )

    tiles(0, POINTS[4], second_sweep)
    copy = to_half(v4b, POINTS[4])
    when(h == 1, copy.wait_recv)

    def last_resid(p, acc):
        now = [v4b[p + 1, t] for t in range(3)]
        scaled = sm[3, 1]
        r = (g4[p, 1] - (1.0 + 4.0 * scaled) * now[1]) + (scaled * around3(now, 1) + v4b[p, 1])
        return acc + r * r

    sc["acc"][4] = lax.fori_loop(0, POINTS[4], last_resid, zero)

    for level, v, g, c, new in ((3, v3, g3, v4b, n3), (2, v2, g2, n3, n2)):
        def ascend(q, level=level, v=v, g=g, c=c, new=new):
            this = [c[q + 1, t] for t in range(3)]
            before = [v[2 * q, t] + c[q, t] for t in range(3)]
            for i in range(2):
                p = 2 * q + i
                now = [v[p + 1, t] + this[t] for t in range(3)]
                for t in range(3):
                    new[p + 1, t] = 0.2 * now[t] + em[level - 1, t] * (
                        g[p, t] + sm[level - 1, t] * around3(now, t) + before[t]
                    )
                before = now

        tiles(0, POINTS[level] // 2, ascend)
        copy = to_half(new, POINTS[level])
        when(h == 1, copy.wait_recv)
    no = sc["no"]

    def ascend1(q):
        scaled, e = sm[0, 1], em[0, 1]
        this, top, bottom = n2[q + 1, 1], n2[q + 1, 0], n2[q + 1, 2]
        before = v1[2 * q] + n2[q, 1]
        for i in range(2):
            p = 2 * q + i
            now = v1[p + 1] + this
            around_it = nb(now, ht[p] + top, hb[p] + bottom)
            no[p] = 0.2 * now + e * (g1[p] + scaled * around_it + before)
            before = now

    tiles(0, POINTS[1] // 2, ascend1)

    def back(r):
        p = (r + GROUP - b) % GROUP
        after = h * GROUP + p + 1
        tile = b + 1

        def keep():
            n1[tile] = no[p]

        def keep_prev():
            np_[tile] = no[p]

        copy = remote(no.at[p], n1.at[tile], sc["bs"], sc["br"].at[b], (h * GROUP + p, s))
        when(p == j, keep)
        when(p != j, copy.start)
        ahead = remote(no.at[p], np_.at[tile], sc["cs"], sc["fr"], (after % (GROUP * HALVES), s))
        crosses = (p % 2 == 1) & (after < GROUP * HALVES)
        when(crosses & (after == m), keep_prev)
        when(crosses & (after != m), ahead.start)

    for part in p_copies[2:]:
        when(far_next & (h == 0), part.start)
    tiles(0, GROUP, back)
    for part in x_copies[:2]:
        when(far_next & (h == 0), part.start)
    for part in x_copies[2:]:
        when(far_next, part.start)

    when(even, level0_again)

    def start_x():
        for copy in x_copies:
            copy.start()

    when(even, start_x)
    for copy in give_copies[6:]:
        when(has_prev, copy.wait_recv)

    def carry_over(i):
        vp[i] = ((ui[i] - wi[i]) + 0.8 * pe[i]) - de[i] * around(wi, i)

    tiles(0, EXT, carry_over)

    def energy(i, acc):
        r0 = ra[i] + (ui[i] - wi[i])
        r1 = rb[i] + wi[i]
        return acc + (r0 * r0 + r1 * r1)

    sc["acc"][0] = lax.fori_loop(1, TILES + 1, energy, zero)

    forward_edges = [
        remote(n1.at[tile], np_.at[tile], sc["ws"].at[k], sc["wr"].at[k], next_id)
        for k, tile in enumerate((0, EXT - 1))
    ]

    def forward(tile):
        return remote(n1.at[tile], np_.at[tile], sc["fs"], sc["fr"], next_id)

    edge_north = remote(n1.at[1], n1.at[EXT - 1], sc["es"].at[0], sc["er"].at[0], north_id)
    edge_south = remote(n1.at[TILES], n1.at[0], sc["es"].at[1], sc["er"].at[1], south_id)

    def correct(i):
        t = n1[i]
        va[i] = va[i] + t
        vb[i] = vb[i] + t

    def arrive(r):
        i = (r + GROUP - j) % GROUP
        copy = remote(n1.at[i + 1], n1.at[i + 1], sc["bs"], sc["br"].at[i], next_id)
        when(i != b, copy.wait_recv)
        when(even, forward(i + 1).start)
        when((i == 0) & (s > 0), edge_north.start)
        when((i == TILES - 1) & (s < STRIPS - 1), edge_south.start)
        correct(i + 1)

    tiles(0, TILES, arrive)
    def some(n, name):
        at = pl.ds(0, n)
        return remote(n1.at[at], np_.at[at], sc[name], sc["fr"], next_id)

    inside = even & (j > 0)
    when(has_prev & jnp.logical_not(inside), some(TILES, "fs").wait_recv)
    when(inside, some(TILES - 1, "fs").wait_recv)

    def last_sweep(i):
        e, d = ee[i], de[i]
        a, bb = va[i], vb[i]
        ra[i] = 0.2 * a + e * (fe[0, i] + d * around(va, i) + (vp[i] + np_[i]))
        rb[i] = 0.2 * bb + e * (fe[1, i] + d * around(vb, i) + a)

    def final(i, acc):
        e, d = ee[i], de[i]
        diag = 1.0 + 4.0 * d
        a, bb, t = ra[i], rb[i], np_[i]
        before = xi[i] + (0.2 * t + e * (d * around(np_, i) + t))
        r0 = (fe[0, i] - diag * a) + (d * around(ra, i) + before)
        r1 = (fe[1, i] - diag * bb) + (d * around(rb, i) + a)
        return acc + (r0 * r0 + r1 * r1)

    tiles(2, TILES, last_sweep)
    for copy in x_copies:
        when(has_prev, copy.wait_recv)
    acc = lax.fori_loop(3, TILES - 1, final, zero)

    when(s < STRIPS - 1, edge_north.wait_recv)
    when(s > 0, edge_south.wait_recv)
    when(has_next, forward_edges[0].start)
    when(has_next, forward_edges[1].start)
    for i in (0, EXT - 1):
        correct(i)
    for copy in forward_edges:
        when(has_prev, copy.wait_recv)
    for i in (0, 1, TILES, EXT - 1):
        last_sweep(i)
    writes = [
        pltpu.make_async_copy(ra.at[inner], out.at[0], sc["write"].at[0]),
        pltpu.make_async_copy(rb.at[inner], out.at[1], sc["write"].at[1]),
    ]
    for write in writes:
        write.start()
    for i in (1, 2, TILES - 1, TILES):
        acc = final(i, acc)
    sc["acc"][5] = acc

    lines = lax.broadcasted_iota(jnp.int32, (8, 128), 0)
    part = jnp.zeros((8, 128), f32)
    for k in range(6):
        whole_sum = sc["acc"][k]
        narrow = whole_sum[:, 0:128]
        for c in range(1, COLS // 128):
            narrow = narrow + whole_sum[:, c * 128:(c + 1) * 128]
        part = jnp.where(lines == k, jnp.sum(narrow, axis=0, keepdims=True), part)
    sc["t0"][...] = part
    sc["q0"][j] = part

    def tell(r, carry):
        copy = remote(sc["t0"], sc["q0"].at[j], sc["ns"].at[0], sc["nr"].at[0], (h * GROUP + (j + r) % GROUP, s))
        copy.start()
        return carry

    lax.fori_loop(1, GROUP, tell, 0)
    heard = remote(sc["q0"].at[pl.ds(0, GROUP - 1)], sc["q0"].at[pl.ds(0, GROUP - 1)], sc["ns"].at[0], sc["nr"].at[0], next_id)
    heard.wait_recv()
    part = sc["q0"][0]
    for k in range(1, GROUP):
        part = part + sc["q0"][k]
    sc["t1"][...] = part
    sc["q1"][mine] = part

    def tell_far(r, carry):
        other = (mine + r) % (HALVES * STRIPS)
        device = ((other // STRIPS) * GROUP + j, other % STRIPS)
        remote(sc["t1"], sc["q1"].at[mine], sc["ns"].at[1], sc["nr"].at[1], device).start()
        return carry

    lax.fori_loop(1, HALVES * STRIPS, tell_far, 0)
    far = pl.ds(0, HALVES * STRIPS - 1)
    heard_far = remote(sc["q1"].at[far], sc["q1"].at[far], sc["ns"].at[1], sc["nr"].at[1], next_id)
    heard_far.wait_recv()
    part = sc["q1"][0]
    for k in range(1, HALVES * STRIPS):
        part = part + sc["q1"][k]
    total = jnp.sum(part, axis=1, keepdims=True)
    norms[...] = jnp.broadcast_to(jnp.sqrt(total / CELLS), (8, 128))

    for copy in give_copies + p_copies + x_copies:
        when(has_next, copy.wait_send)
    for sends, _, copy in sides + wide:
        when(sends, copy.wait_send)
    for copy in halves:
        when(h == 0, copy.wait_send)
    all_in.wait_send()
    remote(no.at[pl.ds(0, GROUP - 1)], no.at[pl.ds(0, GROUP - 1)], sc["bs"], sc["br"].at[0], next_id).wait_send()
    when(even, some(TILES, "fs").wait_send)
    for copy in forward_edges:
        when(has_next, copy.wait_send)
    for half in range(HALVES):
        when((h == half) & inside, some(GROUP // 2 - 1 - half, "cs").wait_send)
        when((h == half) & jnp.logical_not(inside), some(GROUP // 2 - half, "cs").wait_send)
    when(s > 0, edge_north.wait_send)
    when(s < STRIPS - 1, edge_south.wait_send)
    heard.wait_send()
    heard_far.wait_send()
    for write in writes:
        write.wait()


def scratch():
    ext = pltpu.VMEM((EXT, 8, COLS), f32)
    shapes = {"fe": pltpu.VMEM((2, EXT, 8, COLS), f32), "ge": pltpu.VMEM((2, EXT, 8, COLS), f32)}
    for name in ("de", "ee", "va", "vb", "ra", "rb", "uo", "ui", "pe", "xo", "xi", "vp", "wo", "wi", "n1", "np"):
        shapes[name] = ext
    for name in ("g1", "go", "no"):
        shapes[name] = pltpu.VMEM((GROUP, 8, COLS), f32)
    for name, level in (("g2", 2), ("g3", 3), ("g4", 4)):
        shapes[name] = pltpu.VMEM((POINTS[level], 3, 8, COLS), f32)
    shapes["v1"] = pltpu.VMEM((POINTS[1] + 1, 8, COLS), f32)
    for name, level in (("v2", 2), ("v3", 3), ("v4a", 4), ("v4b", 4), ("n3", 3), ("n2", 2)):
        shapes[name] = pltpu.VMEM((POINTS[level] + 1, 3, 8, COLS), f32)
    for name in ("st", "sb", "ht", "hb"):
        shapes[name] = pltpu.VMEM((POINTS[1], 1, COLS), f32)
    shapes["em"] = shapes["sm"] = pltpu.VMEM((4, 3, 8, COLS), f32)
    shapes["acc"] = pltpu.VMEM((6, 8, COLS), f32)
    shapes["t0"] = shapes["t1"] = pltpu.VMEM((8, 128), f32)
    shapes["q0"] = pltpu.VMEM((GROUP, 8, 128), f32)
    shapes["q1"] = pltpu.VMEM((HALVES * STRIPS, 8, 128), f32)
    for name, dims in (
        ("load", (4,)), ("hs", (5, 2)), ("hr", (5, 2)), ("us", (8,)), ("ur", (8,)),
        ("gs", ()), ("gr", ()), ("xs", (7,)), ("xr", (7,)), ("ys", (4,)), ("yr", (4,)), ("cs", ()), ("ws", (2,)), ("wr", (2,)), ("ps", (4,)), ("pr", (4,)),
        ("qs", (4,)), ("qr", (4,)), ("bs", ()), ("br", (TILES,)), ("fs", ()), ("fr", ()),
        ("es", (2,)), ("er", (2,)), ("ns", (2,)), ("nr", (2,)), ("write", (2,)),
    ):
        shapes[name] = pltpu.SemaphoreType.DMA(dims)
    return shapes


def body(rhs, guess, diffusion):
    anywhere = pl.BlockSpec(memory_space=pl.ANY)
    field, norms = pl.pallas_call(
        kernel,
        out_shape=(
            jax.ShapeDtypeStruct((2, TILES, 8, COLS), f32),
            jax.ShapeDtypeStruct((8, 128), f32),
        ),
        in_specs=[anywhere] * 3,
        out_specs=(anywhere, pl.BlockSpec(memory_space=pltpu.VMEM)),
        scratch_shapes=[scratch()],
        compiler_params=pltpu.CompilerParams(collective_id=0, has_side_effects=True, vmem_limit_bytes=60000 * 1024),
        name="cycle",
    )(
        rhs.reshape(2, TILES, 8, COLS),
        guess.reshape(2, TILES, 8, COLS),
        diffusion.reshape(TILES, 8, COLS),
    )
    return field.reshape(2, TILES * 8, COLS), norms[:6, 0]


def solution(mesh):
    return jax.shard_map(
        body,
        mesh=mesh,
        in_specs=(P("tm", "space", None), P("tm", "space", None), P("space", None)),
        out_specs=(P("tm", "space", None), P()),
        check_vma=False,
    )
```

```python
import jax
import jax.numpy as jnp
from jax import lax
from jax.experimental import pallas as pl
from jax.experimental.pallas import tpu as pltpu
from jax.sharding import PartitionSpec as P

MESH = pl.DeviceIdType.MESH
f32 = jnp.float32
GROUP = 32
HALVES = 2
STRIPS = 4
TILES = 32
EXT = TILES + 2
COLS = 1024
CELLS = 1048576.0
POINTS = {1: 32, 2: 16, 3: 8, 4: 4}


def snake(j):
    y = j // 8
    x = (j // 2 + 2) % 4
    x = x + (y % 2) * (3 - 2 * x)
    return (y * 4 + x) * 2 + j % 2


def kernel(rhs, guess, diff, out, norms, sc):
    m = lax.axis_index("tm")
    s = lax.axis_index("space")
    j = m % GROUP
    h = m // GROUP
    odd = s % 2

    def mirror(j, h):
        return j + h * 8 * (3 - 2 * (j // 8))

    def rank_of(b, h=h):
        return mirror(snake(b + odd * (TILES - 1 - 2 * b)), h)

    place = snake(mirror(j, h))
    b = place + odd * (TILES - 1 - 2 * place)
    first = (TILES - 1 - b) // (TILES - 1)
    last = b // (TILES - 1)
    up_id = (h * GROUP + rank_of(b - 1 + first), (s - first + STRIPS) % STRIPS)
    dn_id = (h * GROUP + rank_of(b + 1 - last), (s + last) % STRIPS)
    has_up = b + s > 0
    has_dn = b + s < TILES + STRIPS - 2
    next_id = ((m + 1) % (GROUP * HALVES), s)
    half_id = ((1 - h) * GROUP + rank_of(b, 1 - h), s)
    north_id = (m, (s + STRIPS - 1) % STRIPS)
    south_id = (m, (s + 1) % STRIPS)
    has_next = m < GROUP * HALVES - 1
    has_prev = m > 0

    row = lax.broadcasted_iota(jnp.int32, (8, COLS), 0)
    col = lax.broadcasted_iota(jnp.int32, (8, COLS), 1)

    def nb(tile, above, below):
        up = pltpu.roll(jnp.where(row == 7, above, tile), 1, 0)
        down = pltpu.roll(jnp.where(row == 0, below, tile), 7, 0)
        left = jnp.where(col == 0, 0.0, pltpu.roll(tile, 1, 1))
        right = jnp.where(col == COLS - 1, 0.0, pltpu.roll(tile, COLS - 1, 1))
        return (up + down) + (left + right)

    def around(ref, i):
        return nb(ref[i], ref[i - 1 + (EXT - 1 - i) // (EXT - 1)], ref[i + 1 - i // (EXT - 1)])

    def tiles(lo, hi, fn):
        def step(i, carry):
            fn(i)
            return carry

        lax.fori_loop(lo, hi, step, 0)

    def remote(src, dst, send, recv, device):
        return pltpu.make_async_remote_copy(
            src_ref=src, dst_ref=dst, send_sem=send, recv_sem=recv,
            device_id=device, device_id_type=MESH,
        )

    def when(cond, fn):
        pl.when(cond)(fn)

    fe, ge, de, ee = sc["fe"], sc["ge"], sc["de"], sc["ee"]
    va, vb, ra, rb = sc["va"], sc["vb"], sc["ra"], sc["rb"]
    uo, ui, pe, xo, xi, vp = sc["uo"], sc["ui"], sc["pe"], sc["xo"], sc["xi"], sc["vp"]
    wo, n1, np_ = sc["wo"], sc["n1"], sc["np"]

    inner = pl.ds(1, TILES)
    loads = [
        pltpu.make_async_copy(guess.at[1], ge.at[1, inner], sc["load"].at[0]),
        pltpu.make_async_copy(diff, de.at[inner], sc["load"].at[1]),
        pltpu.make_async_copy(guess.at[0], ge.at[0, inner], sc["load"].at[2]),
        pltpu.make_async_copy(rhs, fe.at[:, inner], sc["load"].at[3]),
    ]
    for load in loads:
        load.start()

    barrier = pltpu.get_barrier_semaphore()

    def greet(device):
        pl.semaphore_signal(barrier, inc=1, device_id=device, device_id_type=MESH)

    def greet_rank(r, carry):
        greet((h * GROUP + (j + r) % GROUP, s))
        return carry

    lax.fori_loop(1, GROUP, greet_rank, 0)
    mine = h * STRIPS + s

    def greet_other(r, carry):
        other = (mine + r) % (HALVES * STRIPS)
        greet(((other // STRIPS) * GROUP + j, other % STRIPS))
        return carry

    lax.fori_loop(1, HALVES * STRIPS, greet_other, 0)
    greet(half_id)
    def greet_first_half():
        def greet_one(r, carry):
            greet((r, s))
            return carry

        lax.fori_loop(1, GROUP, greet_one, 0)

    when(m == GROUP, greet_first_half)

    zero = jnp.zeros((8, COLS), f32)

    def outside(at):
        for ref in (ge.at[1], de, ge.at[0], fe.at[0], fe.at[1], n1):
            ref[at] = zero

    when(s == 0, lambda: outside(0))
    when(s == STRIPS - 1, lambda: outside(EXT - 1))

    def no_prev():
        def clear(i):
            for ref in (ui, pe, xi, np_):
                ref[i] = zero

        tiles(0, EXT, clear)

    when(m == 0, no_prev)

    def no_half():
        sc["v1"][0] = zero
        for name in ("v2", "v3", "v4a", "v4b", "n3", "n2"):
            for t in range(3):
                sc[name][0, t] = zero

    when(h == 0, no_half)

    def no_top():
        def clear(p):
            sc["ht"][p] = jnp.zeros((1, COLS), f32)

        tiles(0, POINTS[1], clear)

        def clear2(p):
            sc["g2"][p, 0] = zero

        tiles(0, POINTS[2], clear2)

    def no_bottom():
        def clear(p):
            sc["hb"][p] = jnp.zeros((1, COLS), f32)

        tiles(0, POINTS[1], clear)

        def clear2(p):
            sc["g2"][p, 2] = zero

        tiles(0, POINTS[2], clear2)

    when(b + s == 0, no_top)
    when(b + s == TILES + STRIPS - 2, no_bottom)

    for load in loads:
        load.wait()

    def damp(i):
        e = 0.8 / (1.0 + 4.0 * de[i])
        ee[i] = e
        wo[i] = e * ge[1, i]

    def sweep_a(i):
        va[i] = 0.2 * ge[0, i] + ee[i] * (fe[0, i] + de[i] * around(ge.at[0], i))

    def sweep_b(i):
        vb[i] = 0.2 * ge[1, i] + ee[i] * (fe[1, i] + de[i] * around(ge.at[1], i) + ge[0, i])

    def give(i):
        uo[i] = (vb[i] - 0.8 * ge[1, i]) + (de[i] * around(wo, i) + wo[i])

    def resid0(i):
        d = de[i]
        diag = 1.0 + 4.0 * d
        a, bb = va[i], vb[i]
        ra[i] = (fe[0, i] - diag * a) + d * around(va, i)
        rb[i] = (fe[1, i] - diag * bb) + (d * around(vb, i) + a)

    spans = ((3, 7), (10, 7), (17, 7), (24, 7), (1, 2), (31, 2), (0, 1), (EXT - 1, 1))
    give_copies = []
    for k, (lo, n) in enumerate(spans):
        at = pl.ds(lo, n)
        give_copies.append(remote(uo.at[at], ui.at[at], sc["us"].at[k], sc["ur"].at[k], next_id))

    def inner_span(k):
        lo, n = spans[k]
        end = lo + n + (k == 3)
        tiles(1 if k == 0 else lo + 1, end + 1, damp)
        tiles(2 if k == 0 else lo, end, sweep_b)
        tiles(lo, lo + n, give)

    inner_span(0)

    peers = GROUP - 1 + HALVES * STRIPS - 1 + 1
    extra = (h == 0) & (j > 0)
    when(extra, lambda: pl.semaphore_wait(barrier, peers + 1))
    when(jnp.logical_not(extra), lambda: pl.semaphore_wait(barrier, peers))

    halo = []
    for k, ref in enumerate((ge.at[1], de, ge.at[0], fe.at[0], fe.at[1])):
        halo.append((
            remote(ref.at[1], ref.at[EXT - 1], sc["hs"].at[k, 0], sc["hr"].at[k, 0], north_id),
            remote(ref.at[TILES], ref.at[0], sc["hs"].at[k, 1], sc["hr"].at[k, 1], south_id),
        ))
    for north, south in halo:
        when(s > 0, north.start)
        when(s < STRIPS - 1, south.start)
    when(has_next, give_copies[0].start)
    for k in range(1, 4):
        inner_span(k)
        when(has_next, give_copies[k].start)
    tiles(2, TILES, sweep_a)
    tiles(3, TILES - 1, resid0)

    def land_halo(pairs):
        for north, south in pairs:
            when(s > 0, north.wait_send)
            when(s < STRIPS - 1, north.wait_recv)
            when(s < STRIPS - 1, south.wait_send)
            when(s > 0, south.wait_recv)

    land_halo(halo[:2])
    damp(0)
    damp(EXT - 1)

    def no_row(at):
        ee[at] = zero
        wo[at] = zero

    when(s == 0, lambda: no_row(0))
    when(s == STRIPS - 1, lambda: no_row(EXT - 1))
    sweep_b(1)
    sweep_b(TILES)
    tiles(1, 3, give)
    when(has_next, give_copies[4].start)
    tiles(TILES - 1, TILES + 1, give)
    when(has_next, give_copies[5].start)
    land_halo(halo[2:])
    for i in (0, EXT - 1):
        sweep_b(i)
        sweep_a(i)
        give(i)
    when(has_next, give_copies[6].start)
    when(has_next, give_copies[7].start)
    sweep_a(1)
    sweep_a(TILES)

    g1, go = sc["g1"], sc["go"]
    tiles(1, 3, resid0)
    tiles(TILES - 1, TILES + 1, resid0)

    def scatter(i):
        g = (ra[i] + rb[i]) + ui[i]
        go[i - 1] = g
        rank = rank_of(i - 1)

        def keep():
            g1[j] = g

        when(rank == j, keep)
        copy = remote(go.at[i - 1], g1.at[j], sc["gs"], sc["gr"], (h * GROUP + rank, s))
        when(rank != j, copy.start)

    for copy, (lo, n) in zip(give_copies[:6], spans):
        when(has_prev, copy.wait_recv)

        def turn(r, lo=lo, n=n):
            scatter(lo + (b + r) % n)

        tiles(0, n, turn)

    even = m % 2 == 0
    wi = sc["wi"]
    parts = ((0, 9), (9, 9), (18, 8), (26, 8))
    p_copies = []
    x_copies = []
    for k, (lo, n) in enumerate(parts):
        at = pl.ds(lo, n)
        p_copies.append(remote(ge.at[1, at], pe.at[at], sc["ps"].at[k], sc["pr"].at[k], next_id))
        x_copies.append(remote(xo.at[at], xi.at[at], sc["qs"].at[k], sc["qr"].at[k], next_id))

    def complete(i):
        w = ee[i] * pe[i]
        va[i] = va[i] + w
        wi[i] = w

    def hand_on(i):
        xo[i] = 0.2 * vb[i] + ee[i] * (fe[1, i] + de[i] * around(vb, i) + va[i])

    def level0_again():
        for copy in p_copies:
            when(has_prev, copy.wait_recv)
        tiles(0, EXT, complete)
        tiles(0, EXT, hand_on)

    def start_p():
        for copy in p_copies:
            copy.start()

    when(even, start_p)
    odd_one = jnp.logical_not(even)
    when(odd_one, level0_again)
    far_next = odd_one & has_next

    em, sm = sc["em"], sc["sm"]
    for t in range(3):
        d = de[b + t]
        for level in range(1, 5):
            em[level - 1, t] = 0.8 / (1.0 + 4.0 * (2.0**level * d))
            sm[level - 1, t] = 2.0**level * d

    def no_damp(t):
        for level in range(1, 5):
            em[level - 1, t] = zero

    when(b + s == 0, lambda: no_damp(0))
    when(b + s == TILES + STRIPS - 2, lambda: no_damp(2))
    all_in = remote(go.at[pl.ds(0, GROUP - 1)], g1.at[pl.ds(0, GROUP - 1)], sc["gs"], sc["gr"], next_id)
    all_in.wait_recv()

    g2, g3, g4 = sc["g2"], sc["g3"], sc["g4"]
    v1, v2, v3, v4a, v4b = sc["v1"], sc["v2"], sc["v3"], sc["v4a"], sc["v4b"]
    n2, n3, ht, hb = sc["n2"], sc["n3"], sc["ht"], sc["hb"]
    halves = []

    def to_half(ref, count):
        k = len(halves)
        copy = remote(ref.at[count], ref.at[0], sc["xs"].at[k], sc["xr"].at[k], half_id)
        halves.append(copy)
        when(h == 0, copy.start)
        return copy

    def first_sweep(p):
        v = em[0, 1] * g1[p]
        v1[p + 1] = v
        sc["st"][p] = v[0:1]
        sc["sb"][p] = v[7:8]

    tiles(0, POINTS[1], first_sweep)
    sides = [
        (has_up, has_dn, remote(sc["st"], hb, sc["ys"].at[0], sc["yr"].at[0], up_id)),
        (has_dn, has_up, remote(sc["sb"], ht, sc["ys"].at[1], sc["yr"].at[1], dn_id)),
    ]

    def start(copies):
        for sends, _, copy in copies:
            when(sends, copy.start)

    def land(copies):
        for _, takes, copy in copies:
            when(takes, copy.wait_recv)

    start(sides)
    copy = to_half(v1, POINTS[1])
    land(sides)
    when(h == 1, copy.wait_recv)

    def descend1(q, acc):
        scaled = sm[0, 1]
        p = 2 * q
        before, now, after = v1[p], v1[p + 1], v1[p + 2]
        r0 = (0.2 * g1[p] + scaled * nb(now, ht[p], hb[p])) + before
        r1 = (0.2 * g1[p + 1] + scaled * nb(after, ht[p + 1], hb[p + 1])) + now
        g2[q, 1] = r0 + r1
        return acc + (r0 * r0 + r1 * r1)

    sc["acc"][1] = lax.fori_loop(0, POINTS[2], descend1, zero)
    mine2 = g2.at[:, 1]
    wide = [
        (has_up, has_dn, remote(mine2, g2.at[:, 2], sc["ys"].at[2], sc["yr"].at[2], up_id)),
        (has_dn, has_up, remote(mine2, g2.at[:, 0], sc["ys"].at[3], sc["yr"].at[3], dn_id)),
    ]
    start(wide)
    for part in (p_copies + x_copies)[0:2]:
        when(far_next & (h >= 0), part.start)
    for part in (p_copies + x_copies)[2:4]:
        when(far_next & (h == 1), part.start)
    land(wide)

    def around3(parts, t):
        return nb(parts[t], parts[max(t - 1, 0)], parts[min(t + 1, 2)])

    def sweep2(p):
        for t in range(3):
            v2[p + 1, t] = em[1, t] * g2[p, t]

    tiles(0, POINTS[2], sweep2)
    copy = to_half(v2, POINTS[2])
    when(h == 1, copy.wait_recv)

    for level, v, g, coarse, vc in ((2, v2, g2, g3, v3), (3, v3, g3, g4, v4a)):
        def descend(q, acc, level=level, v=v, g=g, coarse=coarse, vc=vc):
            p = 2 * q
            now = [v[p + 1, t] for t in range(3)]
            after = [v[p + 2, t] for t in range(3)]
            for t in range(3):
                scaled = sm[level - 1, t]
                r0 = (0.2 * g[p, t] + scaled * around3(now, t)) + v[p, t]
                r1 = (0.2 * g[p + 1, t] + scaled * around3(after, t)) + now[t]
                total = r0 + r1
                coarse[q, t] = total
                vc[q + 1, t] = em[level, t] * total
                if t == 1:
                    acc = acc + (r0 * r0 + r1 * r1)
            return acc

        sc["acc"][level] = lax.fori_loop(0, POINTS[level + 1], descend, zero)
        copy = to_half(vc, POINTS[level + 1])
        when(h == 1, copy.wait_recv)
    def second_sweep(p):
        now = [v4a[p + 1, t] for t in range(3)]
        for t in range(3):
            v4b[p + 1, t] = 0.2 * now[t] + em[3, t] * (
                g4[p, t] + sm[3, t] * around3(now, t) + v4a[p, t]
            )

    tiles(0, POINTS[4], second_sweep)
    copy = to_half(v4b, POINTS[4])
    when(h == 1, copy.wait_recv)

    def last_resid(p, acc):
        now = [v4b[p + 1, t] for t in range(3)]
        scaled = sm[3, 1]
        r = (g4[p, 1] - (1.0 + 4.0 * scaled) * now[1]) + (scaled * around3(now, 1) + v4b[p, 1])
        return acc + r * r

    sc["acc"][4] = lax.fori_loop(0, POINTS[4], last_resid, zero)

    for level, v, g, c, new in ((3, v3, g3, v4b, n3), (2, v2, g2, n3, n2)):
        def ascend(q, level=level, v=v, g=g, c=c, new=new):
            this = [c[q + 1, t] for t in range(3)]
            before = [v[2 * q, t] + c[q, t] for t in range(3)]
            for i in range(2):
                p = 2 * q + i
                now = [v[p + 1, t] + this[t] for t in range(3)]
                for t in range(3):
                    new[p + 1, t] = 0.2 * now[t] + em[level - 1, t] * (
                        g[p, t] + sm[level - 1, t] * around3(now, t) + before[t]
                    )
                before = now

        tiles(0, POINTS[level] // 2, ascend)
        copy = to_half(new, POINTS[level])
        when(h == 1, copy.wait_recv)
    no = sc["no"]

    def ascend1(q):
        scaled, e = sm[0, 1], em[0, 1]
        this, top, bottom = n2[q + 1, 1], n2[q + 1, 0], n2[q + 1, 2]
        before = v1[2 * q] + n2[q, 1]
        for i in range(2):
            p = 2 * q + i
            now = v1[p + 1] + this
            around_it = nb(now, ht[p] + top, hb[p] + bottom)
            no[p] = 0.2 * now + e * (g1[p] + scaled * around_it + before)
            before = now

    tiles(0, POINTS[1] // 2, ascend1)

    def back(r):
        p = (r + GROUP - b) % GROUP
        after = h * GROUP + p + 1
        tile = b + 1

        def keep():
            n1[tile] = no[p]

        def keep_prev():
            np_[tile] = no[p]

        copy = remote(no.at[p], n1.at[tile], sc["bs"], sc["br"].at[b], (h * GROUP + p, s))
        when(p == j, keep)
        when(p != j, copy.start)
        ahead = remote(no.at[p], np_.at[tile], sc["cs"], sc["fr"], (after % (GROUP * HALVES), s))
        crosses = (p % 2 == 1) & (after < GROUP * HALVES)
        when(crosses & (after == m), keep_prev)
        when(crosses & (after != m), ahead.start)

    for part in (p_copies + x_copies)[2:4]:
        when(far_next & (h == 0), part.start)
    tiles(0, GROUP, back)
    for part in (p_copies + x_copies)[4:8]:
        when(far_next & (h >= 0), part.start)

    when(even, level0_again)

    def start_x():
        for copy in x_copies:
            copy.start()

    when(even, start_x)
    for copy in give_copies[6:]:
        when(has_prev, copy.wait_recv)

    def carry_over(i):
        vp[i] = ((ui[i] - wi[i]) + 0.8 * pe[i]) - de[i] * around(wi, i)

    tiles(0, EXT, carry_over)

    def energy(i, acc):
        r0 = ra[i] + (ui[i] - wi[i])
        r1 = rb[i] + wi[i]
        return acc + (r0 * r0 + r1 * r1)

    sc["acc"][0] = lax.fori_loop(1, TILES + 1, energy, zero)

    forward_edges = [
        remote(n1.at[tile], np_.at[tile], sc["ws"].at[k], sc["wr"].at[k], next_id)
        for k, tile in enumerate((0, EXT - 1))
    ]

    def forward(tile):
        return remote(n1.at[tile], np_.at[tile], sc["fs"], sc["fr"], next_id)

    edge_north = remote(n1.at[1], n1.at[EXT - 1], sc["es"].at[0], sc["er"].at[0], north_id)
    edge_south = remote(n1.at[TILES], n1.at[0], sc["es"].at[1], sc["er"].at[1], south_id)

    def correct(i):
        t = n1[i]
        va[i] = va[i] + t
        vb[i] = vb[i] + t

    def arrive(r):
        i = (r + GROUP - j) % GROUP
        copy = remote(n1.at[i + 1], n1.at[i + 1], sc["bs"], sc["br"].at[i], next_id)
        when(i != b, copy.wait_recv)
        when(even, forward(i + 1).start)
        when((i == 0) & (s > 0), edge_north.start)
        when((i == TILES - 1) & (s < STRIPS - 1), edge_south.start)
        correct(i + 1)

    tiles(0, TILES, arrive)
    def some(n, name):
        at = pl.ds(0, n)
        return remote(n1.at[at], np_.at[at], sc[name], sc["fr"], next_id)

    inside = even & (j > 0)
    when(has_prev & jnp.logical_not(inside), some(TILES, "fs").wait_recv)
    when(inside, some(TILES - 1, "fs").wait_recv)

    def last_sweep(i):
        e, d = ee[i], de[i]
        a, bb = va[i], vb[i]
        ra[i] = 0.2 * a + e * (fe[0, i] + d * around(va, i) + (vp[i] + np_[i]))
        rb[i] = 0.2 * bb + e * (fe[1, i] + d * around(vb, i) + a)

    def final(i, acc):
        e, d = ee[i], de[i]
        diag = 1.0 + 4.0 * d
        a, bb, t = ra[i], rb[i], np_[i]
        before = xi[i] + (0.2 * t + e * (d * around(np_, i) + t))
        r0 = (fe[0, i] - diag * a) + (d * around(ra, i) + before)
        r1 = (fe[1, i] - diag * bb) + (d * around(rb, i) + a)
        return acc + (r0 * r0 + r1 * r1)

    tiles(2, TILES, last_sweep)
    for copy in x_copies:
        when(has_prev, copy.wait_recv)
    acc = lax.fori_loop(3, TILES - 1, final, zero)

    when(s < STRIPS - 1, edge_north.wait_recv)
    when(s > 0, edge_south.wait_recv)
    when(has_next, forward_edges[0].start)
    when(has_next, forward_edges[1].start)
    for i in (0, EXT - 1):
        correct(i)
    for copy in forward_edges:
        when(has_prev, copy.wait_recv)
    for i in (0, 1, TILES, EXT - 1):
        last_sweep(i)
    writes = [
        pltpu.make_async_copy(ra.at[inner], out.at[0], sc["write"].at[0]),
        pltpu.make_async_copy(rb.at[inner], out.at[1], sc["write"].at[1]),
    ]
    for write in writes:
        write.start()
    for i in (1, 2, TILES - 1, TILES):
        acc = final(i, acc)
    sc["acc"][5] = acc

    lines = lax.broadcasted_iota(jnp.int32, (8, 128), 0)
    part = jnp.zeros((8, 128), f32)
    for k in range(6):
        whole_sum = sc["acc"][k]
        narrow = whole_sum[:, 0:128]
        for c in range(1, COLS // 128):
            narrow = narrow + whole_sum[:, c * 128:(c + 1) * 128]
        part = jnp.where(lines == k, jnp.sum(narrow, axis=0, keepdims=True), part)
    sc["t0"][...] = part
    sc["q0"][j] = part

    def tell(r, carry):
        copy = remote(sc["t0"], sc["q0"].at[j], sc["ns"].at[0], sc["nr"].at[0], (h * GROUP + (j + r) % GROUP, s))
        copy.start()
        return carry

    lax.fori_loop(1, GROUP, tell, 0)
    heard = remote(sc["q0"].at[pl.ds(0, GROUP - 1)], sc["q0"].at[pl.ds(0, GROUP - 1)], sc["ns"].at[0], sc["nr"].at[0], next_id)
    heard.wait_recv()
    part = sc["q0"][0]
    for k in range(1, GROUP):
        part = part + sc["q0"][k]
    sc["t1"][...] = part
    sc["q1"][mine] = part

    def tell_far(r, carry):
        other = (mine + r) % (HALVES * STRIPS)
        device = ((other // STRIPS) * GROUP + j, other % STRIPS)
        remote(sc["t1"], sc["q1"].at[mine], sc["ns"].at[1], sc["nr"].at[1], device).start()
        return carry

    lax.fori_loop(1, HALVES * STRIPS, tell_far, 0)
    far = pl.ds(0, HALVES * STRIPS - 1)
    heard_far = remote(sc["q1"].at[far], sc["q1"].at[far], sc["ns"].at[1], sc["nr"].at[1], next_id)
    heard_far.wait_recv()
    part = sc["q1"][0]
    for k in range(1, HALVES * STRIPS):
        part = part + sc["q1"][k]
    total = jnp.sum(part, axis=1, keepdims=True)
    root = jnp.sqrt(total / CELLS)
    for k in range(6):
        norms[k] = root[k, 0]

    for copy in give_copies + p_copies + x_copies:
        when(has_next, copy.wait_send)
    for sends, _, copy in sides + wide:
        when(sends, copy.wait_send)
    for copy in halves:
        when(h == 0, copy.wait_send)
    all_in.wait_send()
    remote(no.at[pl.ds(0, GROUP - 1)], no.at[pl.ds(0, GROUP - 1)], sc["bs"], sc["br"].at[0], next_id).wait_send()
    when(even, some(TILES, "fs").wait_send)
    for copy in forward_edges:
        when(has_next, copy.wait_send)
    for half in range(HALVES):
        when((h == half) & inside, some(GROUP // 2 - 1 - half, "cs").wait_send)
        when((h == half) & jnp.logical_not(inside), some(GROUP // 2 - half, "cs").wait_send)
    when(s > 0, edge_north.wait_send)
    when(s < STRIPS - 1, edge_south.wait_send)
    heard.wait_send()
    heard_far.wait_send()
    for write in writes:
        write.wait()


def scratch():
    ext = pltpu.VMEM((EXT, 8, COLS), f32)
    shapes = {"fe": pltpu.VMEM((2, EXT, 8, COLS), f32), "ge": pltpu.VMEM((2, EXT, 8, COLS), f32)}
    for name in ("de", "ee", "va", "vb", "ra", "rb", "uo", "ui", "pe", "xo", "xi", "vp", "wo", "wi", "n1", "np"):
        shapes[name] = ext
    for name in ("g1", "go", "no"):
        shapes[name] = pltpu.VMEM((GROUP, 8, COLS), f32)
    for name, level in (("g2", 2), ("g3", 3), ("g4", 4)):
        shapes[name] = pltpu.VMEM((POINTS[level], 3, 8, COLS), f32)
    shapes["v1"] = pltpu.VMEM((POINTS[1] + 1, 8, COLS), f32)
    for name, level in (("v2", 2), ("v3", 3), ("v4a", 4), ("v4b", 4), ("n3", 3), ("n2", 2)):
        shapes[name] = pltpu.VMEM((POINTS[level] + 1, 3, 8, COLS), f32)
    for name in ("st", "sb", "ht", "hb"):
        shapes[name] = pltpu.VMEM((POINTS[1], 1, COLS), f32)
    shapes["em"] = shapes["sm"] = pltpu.VMEM((4, 3, 8, COLS), f32)
    shapes["acc"] = pltpu.VMEM((6, 8, COLS), f32)
    shapes["t0"] = shapes["t1"] = pltpu.VMEM((8, 128), f32)
    shapes["q0"] = pltpu.VMEM((GROUP, 8, 128), f32)
    shapes["q1"] = pltpu.VMEM((HALVES * STRIPS, 8, 128), f32)
    for name, dims in (
        ("load", (4,)), ("hs", (5, 2)), ("hr", (5, 2)), ("us", (8,)), ("ur", (8,)),
        ("gs", ()), ("gr", ()), ("xs", (7,)), ("xr", (7,)), ("ys", (4,)), ("yr", (4,)), ("cs", ()), ("ws", (2,)), ("wr", (2,)), ("ps", (4,)), ("pr", (4,)),
        ("qs", (4,)), ("qr", (4,)), ("bs", ()), ("br", (TILES,)), ("fs", ()), ("fr", ()),
        ("es", (2,)), ("er", (2,)), ("ns", (2,)), ("nr", (2,)), ("write", (2,)),
    ):
        shapes[name] = pltpu.SemaphoreType.DMA(dims)
    return shapes


PIECES = 8


def copy_kernel(source, target, buffer, come, go):
    rows = TILES * 2 // PIECES
    ins, outs = [], []
    for k in range(PIECES):
        at = (k * rows // TILES, pl.ds(k * rows % TILES, rows))
        ins.append(pltpu.make_async_copy(source.at[at], buffer.at[at], come.at[k]))
        outs.append(pltpu.make_async_copy(buffer.at[at], target.at[at], go.at[k]))
    for copy in ins:
        copy.start()
    for copy, onward in zip(ins, outs):
        copy.wait()
        onward.start()
    for copy in outs:
        copy.wait()


def body(rhs, guess, diffusion):
    anywhere = pl.BlockSpec(memory_space=pl.ANY)
    field, norms = pl.pallas_call(
        kernel,
        out_shape=(
            jax.ShapeDtypeStruct((2, TILES, 8, COLS), f32),
            jax.ShapeDtypeStruct((6,), f32),
        ),
        in_specs=[anywhere] * 3,
        out_specs=(anywhere, pl.BlockSpec(memory_space=pltpu.SMEM)),
        scratch_shapes=[scratch()],
        compiler_params=pltpu.CompilerParams(collective_id=0, has_side_effects=True, vmem_limit_bytes=60000 * 1024),
        name="cycle",
    )(
        rhs.reshape(2, TILES, 8, COLS),
        guess.reshape(2, TILES, 8, COLS),
        diffusion.reshape(TILES, 8, COLS),
    )
    field = pl.pallas_call(
        copy_kernel,
        out_shape=jax.ShapeDtypeStruct(field.shape, f32),
        in_specs=[anywhere],
        out_specs=anywhere,
        scratch_shapes=[
            pltpu.VMEM(field.shape, f32),
            pltpu.SemaphoreType.DMA((PIECES,)),
            pltpu.SemaphoreType.DMA((PIECES,)),
        ],
        compiler_params=pltpu.CompilerParams(vmem_limit_bytes=60000 * 1024),
        name="hand_out",
    )(field)
    return field.reshape(2, TILES * 8, COLS), norms


def solution(mesh):
    return jax.shard_map(
        body,
        mesh=mesh,
        in_specs=(P("tm", "space", None), P("tm", "space", None), P("space", None)),
        out_specs=(P("tm", "space", None), P()),
        check_vma=False,
    )
```

```python
import jax
import jax.numpy as jnp
from jax import lax
from jax.experimental import pallas as pl
from jax.experimental.pallas import tpu as pltpu
from jax.sharding import PartitionSpec as P

MESH = pl.DeviceIdType.MESH
f32 = jnp.float32
GROUP = 32
HALVES = 2
STRIPS = 4
TILES = 32
EXT = TILES + 2
COLS = 1024
CELLS = 1048576.0
POINTS = {1: 32, 2: 16, 3: 8, 4: 4}


def snake(j):
    y = j // 8
    x = (j // 2 + 2) % 4
    x = x + (y % 2) * (3 - 2 * x)
    return (y * 4 + x) * 2 + j % 2


def kernel(rhs, guess, diff, out, norms, sc):
    m = lax.axis_index("tm")
    s = lax.axis_index("space")
    j = m % GROUP
    h = m // GROUP
    odd = s % 2

    def mirror(j, h):
        return j + h * 8 * (3 - 2 * (j // 8))

    def rank_of(b, h=h):
        return mirror(snake(b + odd * (TILES - 1 - 2 * b)), h)

    place = snake(mirror(j, h))
    b = place + odd * (TILES - 1 - 2 * place)
    first = (TILES - 1 - b) // (TILES - 1)
    last = b // (TILES - 1)
    up_id = (h * GROUP + rank_of(b - 1 + first), (s - first + STRIPS) % STRIPS)
    dn_id = (h * GROUP + rank_of(b + 1 - last), (s + last) % STRIPS)
    has_up = b + s > 0
    has_dn = b + s < TILES + STRIPS - 2
    next_id = ((m + 1) % (GROUP * HALVES), s)
    half_id = ((1 - h) * GROUP + rank_of(b, 1 - h), s)
    north_id = (m, (s + STRIPS - 1) % STRIPS)
    south_id = (m, (s + 1) % STRIPS)
    has_next = m < GROUP * HALVES - 1
    has_prev = m > 0

    row = lax.broadcasted_iota(jnp.int32, (8, COLS), 0)
    col = lax.broadcasted_iota(jnp.int32, (8, COLS), 1)

    def nb(tile, above, below):
        up = pltpu.roll(jnp.where(row == 7, above, tile), 1, 0)
        down = pltpu.roll(jnp.where(row == 0, below, tile), 7, 0)
        left = jnp.where(col == 0, 0.0, pltpu.roll(tile, 1, 1))
        right = jnp.where(col == COLS - 1, 0.0, pltpu.roll(tile, COLS - 1, 1))
        return (up + down) + (left + right)

    def around(ref, i):
        return nb(ref[i], ref[i - 1 + (EXT - 1 - i) // (EXT - 1)], ref[i + 1 - i // (EXT - 1)])

    def tiles(lo, hi, fn):
        def step(i, carry):
            fn(i)
            return carry

        lax.fori_loop(lo, hi, step, 0)

    def remote(src, dst, send, recv, device):
        return pltpu.make_async_remote_copy(
            src_ref=src, dst_ref=dst, send_sem=send, recv_sem=recv,
            device_id=device, device_id_type=MESH,
        )

    def when(cond, fn):
        pl.when(cond)(fn)

    fe, ge, de, ee = sc["fe"], sc["ge"], sc["de"], sc["ee"]
    va, vb, ra, rb = sc["va"], sc["vb"], sc["ra"], sc["rb"]
    uo, ui, pe, xo, xi, vp = sc["uo"], sc["ui"], sc["pe"], sc["xo"], sc["xi"], sc["vp"]
    wo, n1, np_ = sc["wo"], sc["n1"], sc["np"]

    inner = pl.ds(1, TILES)
    loads = [
        pltpu.make_async_copy(guess.at[1], ge.at[1, inner], sc["load"].at[0]),
        pltpu.make_async_copy(diff, de.at[inner], sc["load"].at[1]),
        pltpu.make_async_copy(guess.at[0], ge.at[0, inner], sc["load"].at[2]),
        pltpu.make_async_copy(rhs, fe.at[:, inner], sc["load"].at[3]),
    ]
    for load in loads:
        load.start()

    barrier = pltpu.get_barrier_semaphore()

    def greet(device):
        pl.semaphore_signal(barrier, inc=1, device_id=device, device_id_type=MESH)

    def greet_rank(r, carry):
        greet((h * GROUP + (j + r) % GROUP, s))
        return carry

    lax.fori_loop(1, GROUP, greet_rank, 0)
    mine = h * STRIPS + s

    def greet_other(r, carry):
        other = (mine + r) % (HALVES * STRIPS)
        greet(((other // STRIPS) * GROUP + j, other % STRIPS))
        return carry

    lax.fori_loop(1, HALVES * STRIPS, greet_other, 0)
    greet(half_id)
    def greet_first_half():
        def greet_one(r, carry):
            greet((r, s))
            return carry

        lax.fori_loop(1, GROUP, greet_one, 0)

    when(m == GROUP, greet_first_half)

    zero = jnp.zeros((8, COLS), f32)

    def outside(at):
        for ref in (ge.at[1], de, ge.at[0], fe.at[0], fe.at[1], n1):
            ref[at] = zero

    when(s == 0, lambda: outside(0))
    when(s == STRIPS - 1, lambda: outside(EXT - 1))

    def no_prev():
        def clear(i):
            for ref in (ui, pe, xi, np_):
                ref[i] = zero

        tiles(0, EXT, clear)

    when(m == 0, no_prev)

    def no_half():
        sc["v1"][0] = zero
        for name in ("v2", "v3", "v4a", "v4b", "n3", "n2"):
            for t in range(3):
                sc[name][0, t] = zero

    when(h == 0, no_half)

    def no_top():
        def clear(p):
            sc["ht"][p] = jnp.zeros((1, COLS), f32)

        tiles(0, POINTS[1], clear)

        def clear2(p):
            sc["g2"][p, 0] = zero

        tiles(0, POINTS[2], clear2)

    def no_bottom():
        def clear(p):
            sc["hb"][p] = jnp.zeros((1, COLS), f32)

        tiles(0, POINTS[1], clear)

        def clear2(p):
            sc["g2"][p, 2] = zero

        tiles(0, POINTS[2], clear2)

    when(b + s == 0, no_top)
    when(b + s == TILES + STRIPS - 2, no_bottom)

    for load in loads:
        load.wait()

    def damp(i):
        e = 0.8 / (1.0 + 4.0 * de[i])
        ee[i] = e
        wo[i] = e * ge[1, i]

    def sweep_a(i):
        va[i] = 0.2 * ge[0, i] + ee[i] * (fe[0, i] + de[i] * around(ge.at[0], i))

    def sweep_b(i):
        vb[i] = 0.2 * ge[1, i] + ee[i] * (fe[1, i] + de[i] * around(ge.at[1], i) + ge[0, i])

    def give(i):
        uo[i] = (vb[i] - 0.8 * ge[1, i]) + (de[i] * around(wo, i) + wo[i])

    def resid0(i):
        d = de[i]
        diag = 1.0 + 4.0 * d
        a, bb = va[i], vb[i]
        ra[i] = (fe[0, i] - diag * a) + d * around(va, i)
        rb[i] = (fe[1, i] - diag * bb) + (d * around(vb, i) + a)

    spans = ((3, 7), (10, 7), (17, 7), (24, 7), (1, 2), (31, 2), (0, 1), (EXT - 1, 1))
    give_copies = []
    for k, (lo, n) in enumerate(spans):
        at = pl.ds(lo, n)
        give_copies.append(remote(uo.at[at], ui.at[at], sc["us"].at[k], sc["ur"].at[k], next_id))

    def inner_span(k):
        lo, n = spans[k]
        end = lo + n + (k == 3)
        tiles(1 if k == 0 else lo + 1, end + 1, damp)
        tiles(2 if k == 0 else lo, end, sweep_b)
        tiles(lo, lo + n, give)

    inner_span(0)

    peers = GROUP - 1 + HALVES * STRIPS - 1 + 1
    extra = (h == 0) & (j > 0)
    when(extra, lambda: pl.semaphore_wait(barrier, peers + 1))
    when(jnp.logical_not(extra), lambda: pl.semaphore_wait(barrier, peers))

    halo = []
    for k, ref in enumerate((ge.at[1], de, ge.at[0], fe.at[0], fe.at[1])):
        halo.append((
            remote(ref.at[1], ref.at[EXT - 1], sc["hs"].at[k, 0], sc["hr"].at[k, 0], north_id),
            remote(ref.at[TILES], ref.at[0], sc["hs"].at[k, 1], sc["hr"].at[k, 1], south_id),
        ))
    for north, south in halo:
        when(s > 0, north.start)
        when(s < STRIPS - 1, south.start)
    when(has_next, give_copies[0].start)
    for k in range(1, 4):
        inner_span(k)
        when(has_next, give_copies[k].start)
    tiles(2, TILES, sweep_a)
    tiles(3, TILES - 1, resid0)

    def land_halo(pairs):
        for north, south in pairs:
            when(s > 0, north.wait_send)
            when(s < STRIPS - 1, north.wait_recv)
            when(s < STRIPS - 1, south.wait_send)
            when(s > 0, south.wait_recv)

    land_halo(halo[:2])
    damp(0)
    damp(EXT - 1)

    def no_row(at):
        ee[at] = zero
        wo[at] = zero

    when(s == 0, lambda: no_row(0))
    when(s == STRIPS - 1, lambda: no_row(EXT - 1))
    sweep_b(1)
    sweep_b(TILES)
    tiles(1, 3, give)
    when(has_next, give_copies[4].start)
    tiles(TILES - 1, TILES + 1, give)
    when(has_next, give_copies[5].start)
    land_halo(halo[2:])
    for i in (0, EXT - 1):
        sweep_b(i)
        sweep_a(i)
        give(i)
    when(has_next, give_copies[6].start)
    when(has_next, give_copies[7].start)
    sweep_a(1)
    sweep_a(TILES)

    g1, go = sc["g1"], sc["go"]
    tiles(1, 3, resid0)
    tiles(TILES - 1, TILES + 1, resid0)

    def scatter(i):
        g = (ra[i] + rb[i]) + ui[i]
        go[i - 1] = g
        rank = rank_of(i - 1)

        def keep():
            g1[j] = g

        when(rank == j, keep)
        copy = remote(go.at[i - 1], g1.at[j], sc["gs"], sc["gr"], (h * GROUP + rank, s))
        when(rank != j, copy.start)

    for copy, (lo, n) in zip(give_copies[:6], spans):
        when(has_prev, copy.wait_recv)

        def turn(r, lo=lo, n=n):
            scatter(lo + (b + r) % n)

        tiles(0, n, turn)

    even = m % 2 == 0
    wi = sc["wi"]
    parts = ((0, 9), (9, 9), (18, 8), (26, 8))
    p_copies = []
    x_copies = []
    for k, (lo, n) in enumerate(parts):
        at = pl.ds(lo, n)
        p_copies.append(remote(ge.at[1, at], pe.at[at], sc["ps"].at[k], sc["pr"].at[k], next_id))
        x_copies.append(remote(xo.at[at], xi.at[at], sc["qs"].at[k], sc["qr"].at[k], next_id))

    def complete(i):
        w = ee[i] * pe[i]
        va[i] = va[i] + w
        wi[i] = w

    def hand_on(i):
        xo[i] = 0.2 * vb[i] + ee[i] * (fe[1, i] + de[i] * around(vb, i) + va[i])

    def level0_again():
        for copy in p_copies:
            when(has_prev, copy.wait_recv)
        tiles(0, EXT, complete)
        tiles(0, EXT, hand_on)

    def start_p():
        for copy in p_copies:
            copy.start()

    when(even, start_p)
    odd_one = jnp.logical_not(even)
    when(odd_one, level0_again)
    far_next = odd_one & has_next

    em, sm = sc["em"], sc["sm"]
    for t in range(3):
        d = de[b + t]
        for level in range(1, 5):
            em[level - 1, t] = 0.8 / (1.0 + 4.0 * (2.0**level * d))
            sm[level - 1, t] = 2.0**level * d

    def no_damp(t):
        for level in range(1, 5):
            em[level - 1, t] = zero

    when(b + s == 0, lambda: no_damp(0))
    when(b + s == TILES + STRIPS - 2, lambda: no_damp(2))
    all_in = remote(go.at[pl.ds(0, GROUP - 1)], g1.at[pl.ds(0, GROUP - 1)], sc["gs"], sc["gr"], next_id)
    all_in.wait_recv()

    g2, g3, g4 = sc["g2"], sc["g3"], sc["g4"]
    v1, v2, v3, v4a, v4b = sc["v1"], sc["v2"], sc["v3"], sc["v4a"], sc["v4b"]
    n2, n3, ht, hb = sc["n2"], sc["n3"], sc["ht"], sc["hb"]
    halves = []

    def to_half(ref, count, part=None):
        k = len(halves)
        at = () if part is None else (part,)
        copy = remote(ref.at[(count,) + at], ref.at[(0,) + at], sc["xs"].at[k], sc["xr"].at[k], half_id)
        halves.append(copy)
        when(h == 0, copy.start)
        return copy

    def first_sweep(p):
        v = em[0, 1] * g1[p]
        v1[p + 1] = v
        sc["st"][p] = v[0:1]
        sc["sb"][p] = v[7:8]

    tiles(0, POINTS[1], first_sweep)
    sides = [
        (has_up, has_dn, remote(sc["st"], hb, sc["ys"].at[0], sc["yr"].at[0], up_id)),
        (has_dn, has_up, remote(sc["sb"], ht, sc["ys"].at[1], sc["yr"].at[1], dn_id)),
    ]

    def start(copies):
        for sends, _, copy in copies:
            when(sends, copy.start)

    def land(copies):
        for _, takes, copy in copies:
            when(takes, copy.wait_recv)

    start(sides)
    copy = to_half(v1, POINTS[1])
    land(sides)
    when(h == 1, copy.wait_recv)

    def descend1(q, acc):
        scaled = sm[0, 1]
        p = 2 * q
        before, now, after = v1[p], v1[p + 1], v1[p + 2]
        r0 = (0.2 * g1[p] + scaled * nb(now, ht[p], hb[p])) + before
        r1 = (0.2 * g1[p + 1] + scaled * nb(after, ht[p + 1], hb[p + 1])) + now
        g2[q, 1] = r0 + r1
        return acc + (r0 * r0 + r1 * r1)

    sc["acc"][1] = lax.fori_loop(0, POINTS[2], descend1, zero)
    mine2 = g2.at[:, 1]
    wide = [
        (has_up, has_dn, remote(mine2, g2.at[:, 2], sc["ys"].at[2], sc["yr"].at[2], up_id)),
        (has_dn, has_up, remote(mine2, g2.at[:, 0], sc["ys"].at[3], sc["yr"].at[3], dn_id)),
    ]
    start(wide)
    for part in (p_copies + x_copies)[0:2]:
        when(far_next & (h >= 0), part.start)
    for part in (p_copies + x_copies)[2:4]:
        when(far_next & (h == 1), part.start)
    land(wide)

    def around3(parts, t):
        return nb(parts[t], parts[max(t - 1, 0)], parts[min(t + 1, 2)])

    def sweep2(p):
        for t in range(3):
            v2[p + 1, t] = em[1, t] * g2[p, t]

    tiles(0, POINTS[2], sweep2)
    copy = to_half(v2, POINTS[2])
    when(h == 1, copy.wait_recv)

    for level, v, g, coarse, vc in ((2, v2, g2, g3, v3), (3, v3, g3, g4, v4a)):
        def descend(q, acc, level=level, v=v, g=g, coarse=coarse, vc=vc):
            p = 2 * q
            now = [v[p + 1, t] for t in range(3)]
            after = [v[p + 2, t] for t in range(3)]
            for t in range(3):
                scaled = sm[level - 1, t]
                r0 = (0.2 * g[p, t] + scaled * around3(now, t)) + v[p, t]
                r1 = (0.2 * g[p + 1, t] + scaled * around3(after, t)) + now[t]
                total = r0 + r1
                coarse[q, t] = total
                vc[q + 1, t] = em[level, t] * total
                if t == 1:
                    acc = acc + (r0 * r0 + r1 * r1)
            return acc

        sc["acc"][level] = lax.fori_loop(0, POINTS[level + 1], descend, zero)
        copy = to_half(vc, POINTS[level + 1])
        when(h == 1, copy.wait_recv)
    def second_sweep(p):
        now = [v4a[p + 1, t] for t in range(3)]
        for t in range(3):
            v4b[p + 1, t] = 0.2 * now[t] + em[3, t] * (
                g4[p, t] + sm[3, t] * around3(now, t) + v4a[p, t]
            )

    tiles(0, POINTS[4], second_sweep)
    copy = to_half(v4b, POINTS[4])
    when(h == 1, copy.wait_recv)

    def last_resid(p, acc):
        now = [v4b[p + 1, t] for t in range(3)]
        scaled = sm[3, 1]
        r = (g4[p, 1] - (1.0 + 4.0 * scaled) * now[1]) + (scaled * around3(now, 1) + v4b[p, 1])
        return acc + r * r

    sc["acc"][4] = lax.fori_loop(0, POINTS[4], last_resid, zero)

    for level, v, g, c, new in ((3, v3, g3, v4b, n3), (2, v2, g2, n3, n2)):
        def ascend(q, level=level, v=v, g=g, c=c, new=new):
            this = [c[q + 1, t] for t in range(3)]
            before = [v[2 * q, t] + c[q, t] for t in range(3)]
            for i in range(2):
                p = 2 * q + i
                now = [v[p + 1, t] + this[t] for t in range(3)]
                for t in range(3):
                    new[p + 1, t] = 0.2 * now[t] + em[level - 1, t] * (
                        g[p, t] + sm[level - 1, t] * around3(now, t) + before[t]
                    )
                before = now

        tiles(0, POINTS[level] // 2, ascend)
        copy = to_half(new, POINTS[level], 1 if level == 2 else None)
        when(h == 1, copy.wait_recv)
    no = sc["no"]

    def ascend1(q):
        scaled, e = sm[0, 1], em[0, 1]
        this, top, bottom = n2[q + 1, 1], n2[q + 1, 0], n2[q + 1, 2]
        before = v1[2 * q] + n2[q, 1]
        for i in range(2):
            p = 2 * q + i
            now = v1[p + 1] + this
            around_it = nb(now, ht[p] + top, hb[p] + bottom)
            no[p] = 0.2 * now + e * (g1[p] + scaled * around_it + before)
            before = now

    tiles(0, POINTS[1] // 2, ascend1)

    def back(r):
        p = (r + GROUP - b) % GROUP
        after = h * GROUP + p + 1
        tile = b + 1

        def keep():
            n1[tile] = no[p]

        def keep_prev():
            np_[tile] = no[p]

        copy = remote(no.at[p], n1.at[tile], sc["bs"], sc["br"].at[b], (h * GROUP + p, s))
        when(p == j, keep)
        when(p != j, copy.start)
        ahead = remote(no.at[p], np_.at[tile], sc["cs"], sc["fr"], (after % (GROUP * HALVES), s))
        crosses = (p % 2 == 1) & (after < GROUP * HALVES)
        when(crosses & (after == m), keep_prev)
        when(crosses & (after != m), ahead.start)

    for part in (p_copies + x_copies)[2:4]:
        when(far_next & (h == 0), part.start)
    tiles(0, GROUP, back)
    for part in (p_copies + x_copies)[4:8]:
        when(far_next & (h >= 0), part.start)

    when(even, level0_again)

    def start_x():
        for copy in x_copies:
            copy.start()

    when(even, start_x)
    for copy in give_copies[6:]:
        when(has_prev, copy.wait_recv)

    def carry_over(i):
        vp[i] = ((ui[i] - wi[i]) + 0.8 * pe[i]) - de[i] * around(wi, i)

    tiles(0, EXT, carry_over)

    def energy(i, acc):
        r0 = ra[i] + (ui[i] - wi[i])
        r1 = rb[i] + wi[i]
        return acc + (r0 * r0 + r1 * r1)

    sc["acc"][0] = lax.fori_loop(1, TILES + 1, energy, zero)

    forward_edges = [
        remote(n1.at[tile], np_.at[tile], sc["ws"].at[k], sc["wr"].at[k], next_id)
        for k, tile in enumerate((0, EXT - 1))
    ]

    def forward(tile):
        return remote(n1.at[tile], np_.at[tile], sc["fs"], sc["fr"], next_id)

    edge_north = remote(n1.at[1], n1.at[EXT - 1], sc["es"].at[0], sc["er"].at[0], north_id)
    edge_south = remote(n1.at[TILES], n1.at[0], sc["es"].at[1], sc["er"].at[1], south_id)

    def correct(i):
        t = n1[i]
        va[i] = va[i] + t
        vb[i] = vb[i] + t

    def arrive(r):
        i = (r + GROUP - j) % GROUP
        copy = remote(n1.at[i + 1], n1.at[i + 1], sc["bs"], sc["br"].at[i], next_id)
        when(i != b, copy.wait_recv)
        when(even, forward(i + 1).start)
        when((i == 0) & (s > 0), edge_north.start)
        when((i == TILES - 1) & (s < STRIPS - 1), edge_south.start)
        correct(i + 1)

    tiles(0, TILES, arrive)
    def some(n, name):
        at = pl.ds(0, n)
        return remote(n1.at[at], np_.at[at], sc[name], sc["fr"], next_id)

    inside = even & (j > 0)
    when(has_prev & jnp.logical_not(inside), some(TILES, "fs").wait_recv)
    when(inside, some(TILES - 1, "fs").wait_recv)

    def last_sweep(i):
        e, d = ee[i], de[i]
        a, bb = va[i], vb[i]
        ra[i] = 0.2 * a + e * (fe[0, i] + d * around(va, i) + (vp[i] + np_[i]))
        rb[i] = 0.2 * bb + e * (fe[1, i] + d * around(vb, i) + a)

    def final(i, acc):
        e, d = ee[i], de[i]
        diag = 1.0 + 4.0 * d
        a, bb, t = ra[i], rb[i], np_[i]
        before = xi[i] + (0.2 * t + e * (d * around(np_, i) + t))
        r0 = (fe[0, i] - diag * a) + (d * around(ra, i) + before)
        r1 = (fe[1, i] - diag * bb) + (d * around(rb, i) + a)
        return acc + (r0 * r0 + r1 * r1)

    tiles(2, TILES, last_sweep)
    for copy in x_copies:
        when(has_prev, copy.wait_recv)
    acc = lax.fori_loop(3, TILES - 1, final, zero)

    when(s < STRIPS - 1, edge_north.wait_recv)
    when(s > 0, edge_south.wait_recv)
    when(has_next, forward_edges[0].start)
    when(has_next, forward_edges[1].start)
    for i in (0, EXT - 1):
        correct(i)
    for copy in forward_edges:
        when(has_prev, copy.wait_recv)
    for i in (0, 1, TILES, EXT - 1):
        last_sweep(i)
    writes = [
        pltpu.make_async_copy(ra.at[inner], out.at[0], sc["write"].at[0]),
        pltpu.make_async_copy(rb.at[inner], out.at[1], sc["write"].at[1]),
    ]
    for write in writes:
        write.start()
    for i in (1, 2, TILES - 1, TILES):
        acc = final(i, acc)
    sc["acc"][5] = acc

    lines = lax.broadcasted_iota(jnp.int32, (8, 128), 0)
    part = jnp.zeros((8, 128), f32)
    for k in range(6):
        whole_sum = sc["acc"][k]
        narrow = whole_sum[:, 0:128]
        for c in range(1, COLS // 128):
            narrow = narrow + whole_sum[:, c * 128:(c + 1) * 128]
        part = jnp.where(lines == k, jnp.sum(narrow, axis=0, keepdims=True), part)
    sc["t0"][...] = part
    sc["q0"][j] = part

    def tell(r, carry):
        copy = remote(sc["t0"], sc["q0"].at[j], sc["ns"].at[0], sc["nr"].at[0], (h * GROUP + (j + r) % GROUP, s))
        copy.start()
        return carry

    lax.fori_loop(1, GROUP, tell, 0)
    heard = remote(sc["q0"].at[pl.ds(0, GROUP - 1)], sc["q0"].at[pl.ds(0, GROUP - 1)], sc["ns"].at[0], sc["nr"].at[0], next_id)
    heard.wait_recv()
    part = sc["q0"][0]
    for k in range(1, GROUP):
        part = part + sc["q0"][k]
    sc["t1"][...] = part
    sc["q1"][mine] = part

    def tell_far(r, carry):
        other = (mine + r) % (HALVES * STRIPS)
        device = ((other // STRIPS) * GROUP + j, other % STRIPS)
        remote(sc["t1"], sc["q1"].at[mine], sc["ns"].at[1], sc["nr"].at[1], device).start()
        return carry

    lax.fori_loop(1, HALVES * STRIPS, tell_far, 0)
    far = pl.ds(0, HALVES * STRIPS - 1)
    heard_far = remote(sc["q1"].at[far], sc["q1"].at[far], sc["ns"].at[1], sc["nr"].at[1], next_id)
    heard_far.wait_recv()
    part = sc["q1"][0]
    for k in range(1, HALVES * STRIPS):
        part = part + sc["q1"][k]
    total = jnp.sum(part, axis=1, keepdims=True)
    root = jnp.sqrt(total / CELLS)
    for k in range(6):
        norms[k] = root[k, 0]

    for copy in give_copies + p_copies + x_copies:
        when(has_next, copy.wait_send)
    for sends, _, copy in sides + wide:
        when(sends, copy.wait_send)
    for copy in halves:
        when(h == 0, copy.wait_send)
    all_in.wait_send()
    remote(no.at[pl.ds(0, GROUP - 1)], no.at[pl.ds(0, GROUP - 1)], sc["bs"], sc["br"].at[0], next_id).wait_send()
    when(even, some(TILES, "fs").wait_send)
    for copy in forward_edges:
        when(has_next, copy.wait_send)
    for half in range(HALVES):
        when((h == half) & inside, some(GROUP // 2 - 1 - half, "cs").wait_send)
        when((h == half) & jnp.logical_not(inside), some(GROUP // 2 - half, "cs").wait_send)
    when(s > 0, edge_north.wait_send)
    when(s < STRIPS - 1, edge_south.wait_send)
    heard.wait_send()
    heard_far.wait_send()
    for write in writes:
        write.wait()


def scratch():
    ext = pltpu.VMEM((EXT, 8, COLS), f32)
    shapes = {"fe": pltpu.VMEM((2, EXT, 8, COLS), f32), "ge": pltpu.VMEM((2, EXT, 8, COLS), f32)}
    for name in ("de", "ee", "va", "vb", "ra", "rb", "uo", "ui", "pe", "xo", "xi", "vp", "wo", "wi", "n1", "np"):
        shapes[name] = ext
    for name in ("g1", "go", "no"):
        shapes[name] = pltpu.VMEM((GROUP, 8, COLS), f32)
    for name, level in (("g2", 2), ("g3", 3), ("g4", 4)):
        shapes[name] = pltpu.VMEM((POINTS[level], 3, 8, COLS), f32)
    shapes["v1"] = pltpu.VMEM((POINTS[1] + 1, 8, COLS), f32)
    for name, level in (("v2", 2), ("v3", 3), ("v4a", 4), ("v4b", 4), ("n3", 3), ("n2", 2)):
        shapes[name] = pltpu.VMEM((POINTS[level] + 1, 3, 8, COLS), f32)
    for name in ("st", "sb", "ht", "hb"):
        shapes[name] = pltpu.VMEM((POINTS[1], 1, COLS), f32)
    shapes["em"] = shapes["sm"] = pltpu.VMEM((4, 3, 8, COLS), f32)
    shapes["acc"] = pltpu.VMEM((6, 8, COLS), f32)
    shapes["t0"] = shapes["t1"] = pltpu.VMEM((8, 128), f32)
    shapes["q0"] = pltpu.VMEM((GROUP, 8, 128), f32)
    shapes["q1"] = pltpu.VMEM((HALVES * STRIPS, 8, 128), f32)
    for name, dims in (
        ("load", (4,)), ("hs", (5, 2)), ("hr", (5, 2)), ("us", (8,)), ("ur", (8,)),
        ("gs", ()), ("gr", ()), ("xs", (7,)), ("xr", (7,)), ("ys", (4,)), ("yr", (4,)), ("cs", ()), ("ws", (2,)), ("wr", (2,)), ("ps", (4,)), ("pr", (4,)),
        ("qs", (4,)), ("qr", (4,)), ("bs", ()), ("br", (TILES,)), ("fs", ()), ("fr", ()),
        ("es", (2,)), ("er", (2,)), ("ns", (2,)), ("nr", (2,)), ("write", (2,)),
    ):
        shapes[name] = pltpu.SemaphoreType.DMA(dims)
    return shapes


PIECES = 8


def copy_kernel(source, target, buffer, come, go):
    rows = TILES * 2 // PIECES
    ins, outs = [], []
    for k in range(PIECES):
        at = (k * rows // TILES, pl.ds(k * rows % TILES, rows))
        ins.append(pltpu.make_async_copy(source.at[at], buffer.at[at], come.at[k]))
        outs.append(pltpu.make_async_copy(buffer.at[at], target.at[at], go.at[k]))
    for copy in ins:
        copy.start()
    for copy, onward in zip(ins, outs):
        copy.wait()
        onward.start()
    for copy in outs:
        copy.wait()


def body(rhs, guess, diffusion):
    anywhere = pl.BlockSpec(memory_space=pl.ANY)
    field, norms = pl.pallas_call(
        kernel,
        out_shape=(
            jax.ShapeDtypeStruct((2, TILES, 8, COLS), f32),
            jax.ShapeDtypeStruct((6,), f32),
        ),
        in_specs=[anywhere] * 3,
        out_specs=(anywhere, pl.BlockSpec(memory_space=pltpu.SMEM)),
        scratch_shapes=[scratch()],
        compiler_params=pltpu.CompilerParams(collective_id=0, has_side_effects=True, vmem_limit_bytes=60000 * 1024),
        name="cycle",
    )(
        rhs.reshape(2, TILES, 8, COLS),
        guess.reshape(2, TILES, 8, COLS),
        diffusion.reshape(TILES, 8, COLS),
    )
    field = pl.pallas_call(
        copy_kernel,
        out_shape=jax.ShapeDtypeStruct(field.shape, f32),
        in_specs=[anywhere],
        out_specs=anywhere,
        scratch_shapes=[
            pltpu.VMEM(field.shape, f32),
            pltpu.SemaphoreType.DMA((PIECES,)),
            pltpu.SemaphoreType.DMA((PIECES,)),
        ],
        compiler_params=pltpu.CompilerParams(vmem_limit_bytes=60000 * 1024),
        name="hand_out",
    )(field)
    return field.reshape(2, TILES * 8, COLS), norms


def solution(mesh):
    return jax.shard_map(
        body,
        mesh=mesh,
        in_specs=(P("tm", "space", None), P("tm", "space", None), P("space", None)),
        out_specs=(P("tm", "space", None), P()),
        check_vma=False,
    )
```

```python
import jax
import jax.numpy as jnp
from jax import lax
from jax.experimental import pallas as pl
from jax.experimental.pallas import tpu as pltpu
from jax.sharding import PartitionSpec as P

MESH = pl.DeviceIdType.MESH
f32 = jnp.float32
GROUP = 32
HALVES = 2
STRIPS = 4
TILES = 32
EXT = TILES + 2
COLS = 1024
CELLS = 1048576.0
POINTS = {1: 32, 2: 16, 3: 8, 4: 4}


def snake(j):
    y = j // 8
    x = (j // 2 + 2) % 4
    x = x + (y % 2) * (3 - 2 * x)
    return (y * 4 + x) * 2 + j % 2


def kernel(rhs, guess, diff, out, norms, sc):
    m = lax.axis_index("tm")
    s = lax.axis_index("space")
    j = m % GROUP
    h = m // GROUP
    odd = s % 2

    def mirror(j, h):
        return j + h * 8 * (3 - 2 * (j // 8))

    def rank_of(b, h=h):
        return mirror(snake(b + odd * (TILES - 1 - 2 * b)), h)

    place = snake(mirror(j, h))
    b = place + odd * (TILES - 1 - 2 * place)
    first = (TILES - 1 - b) // (TILES - 1)
    last = b // (TILES - 1)
    up_id = (h * GROUP + rank_of(b - 1 + first), (s - first + STRIPS) % STRIPS)
    dn_id = (h * GROUP + rank_of(b + 1 - last), (s + last) % STRIPS)
    has_up = b + s > 0
    has_dn = b + s < TILES + STRIPS - 2
    next_id = ((m + 1) % (GROUP * HALVES), s)
    half_id = ((1 - h) * GROUP + rank_of(b, 1 - h), s)
    north_id = (m, (s + STRIPS - 1) % STRIPS)
    south_id = (m, (s + 1) % STRIPS)
    has_next = m < GROUP * HALVES - 1
    has_prev = m > 0

    row = lax.broadcasted_iota(jnp.int32, (8, COLS), 0)
    col = lax.broadcasted_iota(jnp.int32, (8, COLS), 1)

    def nb(tile, above, below):
        up = pltpu.roll(jnp.where(row == 7, above, tile), 1, 0)
        down = pltpu.roll(jnp.where(row == 0, below, tile), 7, 0)
        left = jnp.where(col == 0, 0.0, pltpu.roll(tile, 1, 1))
        right = jnp.where(col == COLS - 1, 0.0, pltpu.roll(tile, COLS - 1, 1))
        return (up + down) + (left + right)

    def around(ref, i):
        return nb(ref[i], ref[i - 1 + (EXT - 1 - i) // (EXT - 1)], ref[i + 1 - i // (EXT - 1)])

    def tiles(lo, hi, fn):
        def step(i, carry):
            fn(i)
            return carry

        lax.fori_loop(lo, hi, step, 0)

    def remote(src, dst, send, recv, device):
        return pltpu.make_async_remote_copy(
            src_ref=src, dst_ref=dst, send_sem=send, recv_sem=recv,
            device_id=device, device_id_type=MESH,
        )

    def when(cond, fn):
        pl.when(cond)(fn)

    fe, ge, de, ee = sc["fe"], sc["ge"], sc["de"], sc["ee"]
    va, vb, ra, rb = sc["va"], sc["vb"], sc["ra"], sc["rb"]
    uo, ui, pe, xo, xi, vp = sc["uo"], sc["ui"], sc["pe"], sc["xo"], sc["xi"], sc["vp"]
    wo, n1, np_ = sc["wo"], sc["n1"], sc["np"]

    inner = pl.ds(1, TILES)
    loads = [
        pltpu.make_async_copy(guess.at[1], ge.at[1, inner], sc["load"].at[0]),
        pltpu.make_async_copy(diff, de.at[inner], sc["load"].at[1]),
        pltpu.make_async_copy(guess.at[0], ge.at[0, inner], sc["load"].at[2]),
        pltpu.make_async_copy(rhs, fe.at[:, inner], sc["load"].at[3]),
    ]
    for load in loads:
        load.start()

    barrier = pltpu.get_barrier_semaphore()

    def greet(device):
        pl.semaphore_signal(barrier, inc=1, device_id=device, device_id_type=MESH)

    def greet_rank(r, carry):
        greet((h * GROUP + (j + r) % GROUP, s))
        return carry

    lax.fori_loop(1, GROUP, greet_rank, 0)
    mine = h * STRIPS + s

    def greet_other(r, carry):
        other = (mine + r) % (HALVES * STRIPS)
        greet(((other // STRIPS) * GROUP + j, other % STRIPS))
        return carry

    lax.fori_loop(1, HALVES * STRIPS, greet_other, 0)
    greet(half_id)
    def greet_first_half():
        def greet_one(r, carry):
            greet((r, s))
            return carry

        lax.fori_loop(1, GROUP, greet_one, 0)

    when(m == GROUP, greet_first_half)

    zero = jnp.zeros((8, COLS), f32)

    def outside(at):
        for ref in (ge.at[1], de, ge.at[0], fe.at[0], fe.at[1], n1):
            ref[at] = zero

    when(s == 0, lambda: outside(0))
    when(s == STRIPS - 1, lambda: outside(EXT - 1))

    def no_prev():
        def clear(i):
            for ref in (ui, pe, xi, np_):
                ref[i] = zero

        tiles(0, EXT, clear)

    when(m == 0, no_prev)

    def no_half():
        sc["v1"][0] = zero
        for name in ("v2", "v3", "v4a", "v4b", "n3", "n2"):
            for t in range(3):
                sc[name][0, t] = zero

    when(h == 0, no_half)

    def no_top():
        def clear(p):
            sc["ht"][p] = jnp.zeros((1, COLS), f32)

        tiles(0, POINTS[1], clear)

        def clear2(p):
            sc["g2"][p, 0] = zero

        tiles(0, POINTS[2], clear2)

    def no_bottom():
        def clear(p):
            sc["hb"][p] = jnp.zeros((1, COLS), f32)

        tiles(0, POINTS[1], clear)

        def clear2(p):
            sc["g2"][p, 2] = zero

        tiles(0, POINTS[2], clear2)

    when(b + s == 0, no_top)
    when(b + s == TILES + STRIPS - 2, no_bottom)

    for load in loads:
        load.wait()

    def damp(i):
        e = 0.8 / (1.0 + 4.0 * de[i])
        ee[i] = e
        wo[i] = e * ge[1, i]

    def sweep_a(i):
        va[i] = 0.2 * ge[0, i] + ee[i] * (fe[0, i] + de[i] * around(ge.at[0], i))

    def sweep_b(i):
        vb[i] = 0.2 * ge[1, i] + ee[i] * (fe[1, i] + de[i] * around(ge.at[1], i) + ge[0, i])

    def give(i):
        uo[i] = (vb[i] - 0.8 * ge[1, i]) + (de[i] * around(wo, i) + wo[i])

    def resid0(i):
        d = de[i]
        diag = 1.0 + 4.0 * d
        a, bb = va[i], vb[i]
        ra[i] = (fe[0, i] - diag * a) + d * around(va, i)
        rb[i] = (fe[1, i] - diag * bb) + (d * around(vb, i) + a)

    spans = ((3, 7), (10, 7), (17, 7), (24, 7), (1, 2), (31, 2), (0, 1), (EXT - 1, 1))
    give_copies = []
    for k, (lo, n) in enumerate(spans):
        at = pl.ds(lo, n)
        give_copies.append(remote(uo.at[at], ui.at[at], sc["us"].at[k], sc["ur"].at[k], next_id))

    def inner_span(k):
        lo, n = spans[k]
        end = lo + n + (k == 3)
        tiles(1 if k == 0 else lo + 1, end + 1, damp)
        tiles(2 if k == 0 else lo, end, sweep_b)
        tiles(lo, lo + n, give)

    inner_span(0)

    peers = GROUP - 1 + HALVES * STRIPS - 1 + 1
    extra = (h == 0) & (j > 0)
    when(extra, lambda: pl.semaphore_wait(barrier, peers + 1))
    when(jnp.logical_not(extra), lambda: pl.semaphore_wait(barrier, peers))

    halo = []
    for k, ref in enumerate((ge.at[1], de, ge.at[0], fe.at[0], fe.at[1])):
        halo.append((
            remote(ref.at[1], ref.at[EXT - 1], sc["hs"].at[k, 0], sc["hr"].at[k, 0], north_id),
            remote(ref.at[TILES], ref.at[0], sc["hs"].at[k, 1], sc["hr"].at[k, 1], south_id),
        ))
    for north, south in halo:
        when(s > 0, north.start)
        when(s < STRIPS - 1, south.start)
    when(has_next, give_copies[0].start)
    for k in range(1, 4):
        inner_span(k)
        when(has_next, give_copies[k].start)
    tiles(2, TILES, sweep_a)
    tiles(3, TILES - 1, resid0)

    def land_halo(pairs):
        for north, south in pairs:
            when(s > 0, north.wait_send)
            when(s < STRIPS - 1, north.wait_recv)
            when(s < STRIPS - 1, south.wait_send)
            when(s > 0, south.wait_recv)

    land_halo(halo[:2])
    damp(0)
    damp(EXT - 1)

    def no_row(at):
        ee[at] = zero
        wo[at] = zero

    when(s == 0, lambda: no_row(0))
    when(s == STRIPS - 1, lambda: no_row(EXT - 1))
    sweep_b(1)
    sweep_b(TILES)
    tiles(1, 3, give)
    when(has_next, give_copies[4].start)
    tiles(TILES - 1, TILES + 1, give)
    when(has_next, give_copies[5].start)
    land_halo(halo[2:])
    for i in (0, EXT - 1):
        sweep_b(i)
        sweep_a(i)
        give(i)
    when(has_next, give_copies[6].start)
    when(has_next, give_copies[7].start)
    sweep_a(1)
    sweep_a(TILES)

    g1, go = sc["g1"], sc["go"]
    tiles(1, 3, resid0)
    tiles(TILES - 1, TILES + 1, resid0)

    def scatter(i):
        g = (ra[i] + rb[i]) + ui[i]
        go[i - 1] = g
        rank = rank_of(i - 1)

        def keep():
            g1[j] = g

        when(rank == j, keep)
        copy = remote(go.at[i - 1], g1.at[j], sc["gs"], sc["gr"], (h * GROUP + rank, s))
        when(rank != j, copy.start)

    for copy, (lo, n) in zip(give_copies[:6], spans):
        when(has_prev, copy.wait_recv)

        def turn(r, lo=lo, n=n):
            scatter(lo + (b + r) % n)

        tiles(0, n, turn)

    even = m % 2 == 0
    wi = sc["wi"]
    parts = ((0, 9), (9, 9), (18, 8), (26, 8))
    p_copies = []
    x_copies = []
    for k, (lo, n) in enumerate(parts):
        at = pl.ds(lo, n)
        p_copies.append(remote(ge.at[1, at], pe.at[at], sc["ps"].at[k], sc["pr"].at[k], next_id))
        at = pl.ds(1 + k * TILES // 4, TILES // 4)
        x_copies.append(remote(xo.at[at], xi.at[at], sc["qs"].at[k], sc["qr"].at[k], next_id))

    def complete(i):
        w = ee[i] * pe[i]
        va[i] = va[i] + w
        wi[i] = w

    def hand_on(i):
        xo[i] = 0.2 * vb[i] + ee[i] * (fe[1, i] + de[i] * around(vb, i) + va[i])

    def level0_again():
        for copy in p_copies:
            when(has_prev, copy.wait_recv)
        tiles(0, EXT, complete)
        tiles(1, TILES + 1, hand_on)

    def start_p():
        for copy in p_copies:
            copy.start()

    when(even, start_p)
    odd_one = jnp.logical_not(even)
    when(odd_one, level0_again)
    far_next = odd_one & has_next

    em, sm = sc["em"], sc["sm"]
    for t in range(3):
        d = de[b + t]
        for level in range(1, 5):
            em[level - 1, t] = 0.8 / (1.0 + 4.0 * (2.0**level * d))
            sm[level - 1, t] = 2.0**level * d

    def no_damp(t):
        for level in range(1, 5):
            em[level - 1, t] = zero

    when(b + s == 0, lambda: no_damp(0))
    when(b + s == TILES + STRIPS - 2, lambda: no_damp(2))
    all_in = remote(go.at[pl.ds(0, GROUP - 1)], g1.at[pl.ds(0, GROUP - 1)], sc["gs"], sc["gr"], next_id)
    all_in.wait_recv()

    g2, g3, g4 = sc["g2"], sc["g3"], sc["g4"]
    v1, v2, v3, v4a, v4b = sc["v1"], sc["v2"], sc["v3"], sc["v4a"], sc["v4b"]
    n2, n3, ht, hb = sc["n2"], sc["n3"], sc["ht"], sc["hb"]
    halves = []

    def to_half(ref, count, part=None):
        k = len(halves)
        at = () if part is None else (part,)
        copy = remote(ref.at[(count,) + at], ref.at[(0,) + at], sc["xs"].at[k], sc["xr"].at[k], half_id)
        halves.append(copy)
        when(h == 0, copy.start)
        return copy

    def first_sweep(p):
        v = em[0, 1] * g1[p]
        v1[p + 1] = v
        sc["st"][p] = v[0:1]
        sc["sb"][p] = v[7:8]

    tiles(0, POINTS[1], first_sweep)
    sides = [
        (has_up, has_dn, remote(sc["st"], hb, sc["ys"].at[0], sc["yr"].at[0], up_id)),
        (has_dn, has_up, remote(sc["sb"], ht, sc["ys"].at[1], sc["yr"].at[1], dn_id)),
    ]

    def start(copies):
        for sends, _, copy in copies:
            when(sends, copy.start)

    def land(copies):
        for _, takes, copy in copies:
            when(takes, copy.wait_recv)

    start(sides)
    copy = to_half(v1, POINTS[1])
    land(sides)
    when(h == 1, copy.wait_recv)

    def descend1(q, acc):
        scaled = sm[0, 1]
        p = 2 * q
        before, now, after = v1[p], v1[p + 1], v1[p + 2]
        r0 = (0.2 * g1[p] + scaled * nb(now, ht[p], hb[p])) + before
        r1 = (0.2 * g1[p + 1] + scaled * nb(after, ht[p + 1], hb[p + 1])) + now
        g2[q, 1] = r0 + r1
        return acc + (r0 * r0 + r1 * r1)

    sc["acc"][1] = lax.fori_loop(0, POINTS[2], descend1, zero)
    mine2 = g2.at[:, 1]
    wide = [
        (has_up, has_dn, remote(mine2, g2.at[:, 2], sc["ys"].at[2], sc["yr"].at[2], up_id)),
        (has_dn, has_up, remote(mine2, g2.at[:, 0], sc["ys"].at[3], sc["yr"].at[3], dn_id)),
    ]
    start(wide)
    for part in (p_copies + x_copies)[0:2]:
        when(far_next & (h >= 0), part.start)
    for part in (p_copies + x_copies)[2:4]:
        when(far_next & (h == 1), part.start)
    land(wide)

    def around3(parts, t):
        return nb(parts[t], parts[max(t - 1, 0)], parts[min(t + 1, 2)])

    def sweep2(p):
        for t in range(3):
            v2[p + 1, t] = em[1, t] * g2[p, t]

    tiles(0, POINTS[2], sweep2)
    copy = to_half(v2, POINTS[2])
    when(h == 1, copy.wait_recv)

    for level, v, g, coarse, vc in ((2, v2, g2, g3, v3), (3, v3, g3, g4, v4a)):
        def descend(q, acc, level=level, v=v, g=g, coarse=coarse, vc=vc):
            p = 2 * q
            now = [v[p + 1, t] for t in range(3)]
            after = [v[p + 2, t] for t in range(3)]
            for t in range(3):
                scaled = sm[level - 1, t]
                r0 = (0.2 * g[p, t] + scaled * around3(now, t)) + v[p, t]
                r1 = (0.2 * g[p + 1, t] + scaled * around3(after, t)) + now[t]
                total = r0 + r1
                coarse[q, t] = total
                vc[q + 1, t] = em[level, t] * total
                if t == 1:
                    acc = acc + (r0 * r0 + r1 * r1)
            return acc

        sc["acc"][level] = lax.fori_loop(0, POINTS[level + 1], descend, zero)
        copy = to_half(vc, POINTS[level + 1])
        when(h == 1, copy.wait_recv)
    def second_sweep(p):
        now = [v4a[p + 1, t] for t in range(3)]
        for t in range(3):
            v4b[p + 1, t] = 0.2 * now[t] + em[3, t] * (
                g4[p, t] + sm[3, t] * around3(now, t) + v4a[p, t]
            )

    tiles(0, POINTS[4], second_sweep)
    copy = to_half(v4b, POINTS[4])
    when(h == 1, copy.wait_recv)

    def last_resid(p, acc):
        now = [v4b[p + 1, t] for t in range(3)]
        scaled = sm[3, 1]
        r = (g4[p, 1] - (1.0 + 4.0 * scaled) * now[1]) + (scaled * around3(now, 1) + v4b[p, 1])
        return acc + r * r

    sc["acc"][4] = lax.fori_loop(0, POINTS[4], last_resid, zero)

    for level, v, g, c, new in ((3, v3, g3, v4b, n3), (2, v2, g2, n3, n2)):
        def ascend(q, level=level, v=v, g=g, c=c, new=new):
            this = [c[q + 1, t] for t in range(3)]
            before = [v[2 * q, t] + c[q, t] for t in range(3)]
            for i in range(2):
                p = 2 * q + i
                now = [v[p + 1, t] + this[t] for t in range(3)]
                for t in range(3):
                    new[p + 1, t] = 0.2 * now[t] + em[level - 1, t] * (
                        g[p, t] + sm[level - 1, t] * around3(now, t) + before[t]
                    )
                before = now

        tiles(0, POINTS[level] // 2, ascend)
        copy = to_half(new, POINTS[level], 1 if level == 2 else None)
        when(h == 1, copy.wait_recv)
    no = sc["no"]

    def ascend1(q):
        scaled, e = sm[0, 1], em[0, 1]
        this, top, bottom = n2[q + 1, 1], n2[q + 1, 0], n2[q + 1, 2]
        before = v1[2 * q] + n2[q, 1]
        for i in range(2):
            p = 2 * q + i
            now = v1[p + 1] + this
            around_it = nb(now, ht[p] + top, hb[p] + bottom)
            no[p] = 0.2 * now + e * (g1[p] + scaled * around_it + before)
            before = now

    tiles(0, POINTS[1] // 2, ascend1)

    def back(r):
        p = (r + GROUP - b) % GROUP
        after = h * GROUP + p + 1
        tile = b + 1

        def keep():
            n1[tile] = no[p]

        def keep_prev():
            np_[tile] = no[p]

        copy = remote(no.at[p], n1.at[tile], sc["bs"], sc["br"].at[b], (h * GROUP + p, s))
        when(p == j, keep)
        when(p != j, copy.start)
        ahead = remote(no.at[p], np_.at[tile], sc["cs"], sc["fr"], (after % (GROUP * HALVES), s))
        crosses = (p % 2 == 1) & (after < GROUP * HALVES)
        when(crosses & (after == m), keep_prev)
        when(crosses & (after != m), ahead.start)

    for part in (p_copies + x_copies)[2:4]:
        when(far_next & (h == 0), part.start)
    tiles(0, GROUP, back)
    for part in (p_copies + x_copies)[4:8]:
        when(far_next & (h >= 0), part.start)

    when(even, level0_again)

    def start_x():
        for copy in x_copies:
            copy.start()

    when(even, start_x)
    for copy in give_copies[6:]:
        when(has_prev, copy.wait_recv)

    def carry_over(i):
        vp[i] = ((ui[i] - wi[i]) + 0.8 * pe[i]) - de[i] * around(wi, i)

    tiles(0, EXT, carry_over)

    def energy(i, acc):
        r0 = ra[i] + (ui[i] - wi[i])
        r1 = rb[i] + wi[i]
        return acc + (r0 * r0 + r1 * r1)

    sc["acc"][0] = lax.fori_loop(1, TILES + 1, energy, zero)

    forward_edges = [
        remote(n1.at[tile], np_.at[tile], sc["ws"].at[k], sc["wr"].at[k], next_id)
        for k, tile in enumerate((0, EXT - 1))
    ]

    def forward(tile):
        return remote(n1.at[tile], np_.at[tile], sc["fs"], sc["fr"], next_id)

    edge_north = remote(n1.at[1], n1.at[EXT - 1], sc["es"].at[0], sc["er"].at[0], north_id)
    edge_south = remote(n1.at[TILES], n1.at[0], sc["es"].at[1], sc["er"].at[1], south_id)

    def correct(i):
        t = n1[i]
        va[i] = va[i] + t
        vb[i] = vb[i] + t

    def arrive(r):
        i = (r + GROUP - j) % GROUP
        copy = remote(n1.at[i + 1], n1.at[i + 1], sc["bs"], sc["br"].at[i], next_id)
        when(i != b, copy.wait_recv)
        when(even, forward(i + 1).start)
        when((i == 0) & (s > 0), edge_north.start)
        when((i == TILES - 1) & (s < STRIPS - 1), edge_south.start)
        correct(i + 1)

    tiles(0, TILES, arrive)
    def some(n, name):
        at = pl.ds(0, n)
        return remote(n1.at[at], np_.at[at], sc[name], sc["fr"], next_id)

    inside = even & (j > 0)
    when(has_prev & jnp.logical_not(inside), some(TILES, "fs").wait_recv)
    when(inside, some(TILES - 1, "fs").wait_recv)

    def last_sweep(i):
        e, d = ee[i], de[i]
        a, bb = va[i], vb[i]
        ra[i] = 0.2 * a + e * (fe[0, i] + d * around(va, i) + (vp[i] + np_[i]))
        rb[i] = 0.2 * bb + e * (fe[1, i] + d * around(vb, i) + a)

    def final(i, acc):
        e, d = ee[i], de[i]
        diag = 1.0 + 4.0 * d
        a, bb, t = ra[i], rb[i], np_[i]
        before = xi[i] + (0.2 * t + e * (d * around(np_, i) + t))
        r0 = (fe[0, i] - diag * a) + (d * around(ra, i) + before)
        r1 = (fe[1, i] - diag * bb) + (d * around(rb, i) + a)
        return acc + (r0 * r0 + r1 * r1)

    tiles(2, TILES, last_sweep)
    for copy in x_copies:
        when(has_prev, copy.wait_recv)
    acc = lax.fori_loop(3, TILES - 1, final, zero)

    when(s < STRIPS - 1, edge_north.wait_recv)
    when(s > 0, edge_south.wait_recv)
    when(has_next, forward_edges[0].start)
    when(has_next, forward_edges[1].start)
    for i in (0, EXT - 1):
        correct(i)
    for copy in forward_edges:
        when(has_prev, copy.wait_recv)
    for i in (0, 1, TILES, EXT - 1):
        last_sweep(i)
    writes = [
        pltpu.make_async_copy(ra.at[inner], out.at[0], sc["write"].at[0]),
        pltpu.make_async_copy(rb.at[inner], out.at[1], sc["write"].at[1]),
    ]
    for write in writes:
        write.start()
    for i in (1, 2, TILES - 1, TILES):
        acc = final(i, acc)
    sc["acc"][5] = acc

    lines = lax.broadcasted_iota(jnp.int32, (8, 128), 0)
    part = jnp.zeros((8, 128), f32)
    for k in range(6):
        whole_sum = sc["acc"][k]
        narrow = whole_sum[:, 0:128]
        for c in range(1, COLS // 128):
            narrow = narrow + whole_sum[:, c * 128:(c + 1) * 128]
        part = jnp.where(lines == k, jnp.sum(narrow, axis=0, keepdims=True), part)
    sc["t0"][...] = part
    sc["q0"][j] = part

    def tell(r, carry):
        copy = remote(sc["t0"], sc["q0"].at[j], sc["ns"].at[0], sc["nr"].at[0], (h * GROUP + (j + r) % GROUP, s))
        copy.start()
        return carry

    lax.fori_loop(1, GROUP, tell, 0)
    heard = remote(sc["q0"].at[pl.ds(0, GROUP - 1)], sc["q0"].at[pl.ds(0, GROUP - 1)], sc["ns"].at[0], sc["nr"].at[0], next_id)
    heard.wait_recv()
    part = sc["q0"][0]
    for k in range(1, GROUP):
        part = part + sc["q0"][k]
    sc["t1"][...] = part
    sc["q1"][mine] = part

    def tell_far(r, carry):
        other = (mine + r) % (HALVES * STRIPS)
        device = ((other // STRIPS) * GROUP + j, other % STRIPS)
        remote(sc["t1"], sc["q1"].at[mine], sc["ns"].at[1], sc["nr"].at[1], device).start()
        return carry

    lax.fori_loop(1, HALVES * STRIPS, tell_far, 0)
    far = pl.ds(0, HALVES * STRIPS - 1)
    heard_far = remote(sc["q1"].at[far], sc["q1"].at[far], sc["ns"].at[1], sc["nr"].at[1], next_id)
    heard_far.wait_recv()
    part = sc["q1"][0]
    for k in range(1, HALVES * STRIPS):
        part = part + sc["q1"][k]
    total = jnp.sum(part, axis=1, keepdims=True)
    root = jnp.sqrt(total / CELLS)
    for k in range(6):
        norms[k] = root[k, 0]

    for copy in give_copies + p_copies + x_copies:
        when(has_next, copy.wait_send)
    for sends, _, copy in sides + wide:
        when(sends, copy.wait_send)
    for copy in halves:
        when(h == 0, copy.wait_send)
    all_in.wait_send()
    remote(no.at[pl.ds(0, GROUP - 1)], no.at[pl.ds(0, GROUP - 1)], sc["bs"], sc["br"].at[0], next_id).wait_send()
    when(even, some(TILES, "fs").wait_send)
    for copy in forward_edges:
        when(has_next, copy.wait_send)
    for half in range(HALVES):
        when((h == half) & inside, some(GROUP // 2 - 1 - half, "cs").wait_send)
        when((h == half) & jnp.logical_not(inside), some(GROUP // 2 - half, "cs").wait_send)
    when(s > 0, edge_north.wait_send)
    when(s < STRIPS - 1, edge_south.wait_send)
    heard.wait_send()
    heard_far.wait_send()
    for write in writes:
        write.wait()


def scratch():
    ext = pltpu.VMEM((EXT, 8, COLS), f32)
    shapes = {"fe": pltpu.VMEM((2, EXT, 8, COLS), f32), "ge": pltpu.VMEM((2, EXT, 8, COLS), f32)}
    for name in ("de", "ee", "va", "vb", "ra", "rb", "uo", "ui", "pe", "xo", "xi", "vp", "wo", "wi", "n1", "np"):
        shapes[name] = ext
    for name in ("g1", "go", "no"):
        shapes[name] = pltpu.VMEM((GROUP, 8, COLS), f32)
    for name, level in (("g2", 2), ("g3", 3), ("g4", 4)):
        shapes[name] = pltpu.VMEM((POINTS[level], 3, 8, COLS), f32)
    shapes["v1"] = pltpu.VMEM((POINTS[1] + 1, 8, COLS), f32)
    for name, level in (("v2", 2), ("v3", 3), ("v4a", 4), ("v4b", 4), ("n3", 3), ("n2", 2)):
        shapes[name] = pltpu.VMEM((POINTS[level] + 1, 3, 8, COLS), f32)
    for name in ("st", "sb", "ht", "hb"):
        shapes[name] = pltpu.VMEM((POINTS[1], 1, COLS), f32)
    shapes["em"] = shapes["sm"] = pltpu.VMEM((4, 3, 8, COLS), f32)
    shapes["acc"] = pltpu.VMEM((6, 8, COLS), f32)
    shapes["t0"] = shapes["t1"] = pltpu.VMEM((8, 128), f32)
    shapes["q0"] = pltpu.VMEM((GROUP, 8, 128), f32)
    shapes["q1"] = pltpu.VMEM((HALVES * STRIPS, 8, 128), f32)
    for name, dims in (
        ("load", (4,)), ("hs", (5, 2)), ("hr", (5, 2)), ("us", (8,)), ("ur", (8,)),
        ("gs", ()), ("gr", ()), ("xs", (7,)), ("xr", (7,)), ("ys", (4,)), ("yr", (4,)), ("cs", ()), ("ws", (2,)), ("wr", (2,)), ("ps", (4,)), ("pr", (4,)),
        ("qs", (4,)), ("qr", (4,)), ("bs", ()), ("br", (TILES,)), ("fs", ()), ("fr", ()),
        ("es", (2,)), ("er", (2,)), ("ns", (2,)), ("nr", (2,)), ("write", (2,)),
    ):
        shapes[name] = pltpu.SemaphoreType.DMA(dims)
    return shapes


PIECES = 8


def copy_kernel(source, target, buffer, come, go):
    rows = TILES * 2 // PIECES
    ins, outs = [], []
    for k in range(PIECES):
        at = (k * rows // TILES, pl.ds(k * rows % TILES, rows))
        ins.append(pltpu.make_async_copy(source.at[at], buffer.at[at], come.at[k]))
        outs.append(pltpu.make_async_copy(buffer.at[at], target.at[at], go.at[k]))
    for copy in ins:
        copy.start()
    for copy, onward in zip(ins, outs):
        copy.wait()
        onward.start()
    for copy in outs:
        copy.wait()


def body(rhs, guess, diffusion):
    anywhere = pl.BlockSpec(memory_space=pl.ANY)
    field, norms = pl.pallas_call(
        kernel,
        out_shape=(
            jax.ShapeDtypeStruct((2, TILES, 8, COLS), f32),
            jax.ShapeDtypeStruct((6,), f32),
        ),
        in_specs=[anywhere] * 3,
        out_specs=(anywhere, pl.BlockSpec(memory_space=pltpu.SMEM)),
        scratch_shapes=[scratch()],
        compiler_params=pltpu.CompilerParams(collective_id=0, has_side_effects=True, vmem_limit_bytes=60000 * 1024),
        name="cycle",
    )(
        rhs.reshape(2, TILES, 8, COLS),
        guess.reshape(2, TILES, 8, COLS),
        diffusion.reshape(TILES, 8, COLS),
    )
    field = pl.pallas_call(
        copy_kernel,
        out_shape=jax.ShapeDtypeStruct(field.shape, f32),
        in_specs=[anywhere],
        out_specs=anywhere,
        scratch_shapes=[
            pltpu.VMEM(field.shape, f32),
            pltpu.SemaphoreType.DMA((PIECES,)),
            pltpu.SemaphoreType.DMA((PIECES,)),
        ],
        compiler_params=pltpu.CompilerParams(vmem_limit_bytes=60000 * 1024),
        name="hand_out",
    )(field)
    return field.reshape(2, TILES * 8, COLS), norms


def solution(mesh):
    return jax.shard_map(
        body,
        mesh=mesh,
        in_specs=(P("tm", "space", None), P("tm", "space", None), P("space", None)),
        out_specs=(P("tm", "space", None), P()),
        check_vma=False,
    )
```
